8 devices in a mesh: data: 1 (over z), model: 8 (over y, x, core).
Axes of the slice: x: 2, y: 2, z: 1, core: 2. Of those that a mesh axis runs over, the one named last changes fastest.
Arguments:
- act_x: bfloat16 [1536, 5120], P('data')
- seg_ids: int32 [1536], P('data')
- gain_one: bfloat16 [5120], replicated
- gain_two: bfloat16 [5120], replicated
- w_qkv: bfloat16 [5120, 15360], P(None, 'model')
- w_out: bfloat16 [40, 128, 5120], P('model')
- w_up: bfloat16 [5120, 20480], P(None, 'model')
- w_down: bfloat16 [20480, 5120], P('model')
- grad_y: bfloat16 [1536, 5120], P('data')
Outputs:
- output 1: bfloat16 [1536, 5120], P('data')
- output 2: bfloat16 [1536, 5120], P('data')
- output 3: bfloat16 [5120, 15360], P('data', 'model')
- output 4: bfloat16 [40, 128, 5120], P(('data', 'model'))
- output 5: bfloat16 [5120, 20480], P('data', 'model')
- output 6: bfloat16 [20480, 5120], P(('data', 'model'))
- output 7: bfloat16 [5120], P('data')
- output 8: bfloat16 [5120], P('data')
All inputs are finite; a program needn't handle non-finite values.
Results may differ from the reference program's by a relative error of at most 0.02.
Values are sent between devices in bfloat16 or wider.
A program may use at most 1 GiB of HBM per device.

```python
import jax
import jax.numpy as jnp
from jax import lax

HIDDEN = 5120
NUM_HEADS = 40
HEAD_DIM = 128
FFN_DIM = 20480
SEQ_LEN = 1536
NUM_BOUNDS = 3


def matmul_f32(left, right):
    return jnp.dot(left.astype(jnp.float32), right.astype(jnp.float32))


def layer_norm(values, gain_vec):
    values_f32 = values.astype(jnp.float32)
    centered = values_f32 - jnp.mean(values_f32, axis=-1, keepdims=True)
    variance = jnp.mean(centered * centered, axis=-1, keepdims=True)
    return centered * lax.rsqrt(variance + 1e-5) * gain_vec.astype(jnp.float32)


def setup_inputs(seed: int = 0, part: int = 0) -> dict:
    part_key = jax.random.fold_in(jax.random.key(seed), part)
    key_x, key_dy, key_seg = jax.random.split(part_key, 3)
    weight_keys = jax.random.split(jax.random.key(seed + 1), 6)
    act_x = jax.random.normal(key_x, (SEQ_LEN, HIDDEN), jnp.float32)
    grad_y = jax.random.normal(key_dy, (SEQ_LEN, HIDDEN), jnp.float32)
    bounds = jax.random.randint(key_seg, (NUM_BOUNDS,), 1, SEQ_LEN, dtype=jnp.int32)
    positions = jnp.arange(SEQ_LEN, dtype=jnp.int32)
    seg_ids = jnp.sum((positions[:, None] >= bounds[None, :]).astype(jnp.int32), axis=1).astype(jnp.int32)
    gain_one = 1.0 + 0.3 * jax.random.normal(weight_keys[0], (HIDDEN,), jnp.float32)
    gain_two = 1.0 + 0.3 * jax.random.normal(weight_keys[1], (HIDDEN,), jnp.float32)
    part_scale = jnp.array([1.5, 1.5, 1.0], jnp.float32)
    col_scale = jnp.tile(jnp.repeat(part_scale, HEAD_DIM), NUM_HEADS)
    w_qkv = jax.random.normal(weight_keys[2], (HIDDEN, 3 * NUM_HEADS * HEAD_DIM), jnp.float32) * (HIDDEN ** -0.5) * col_scale
    w_out = jax.random.normal(weight_keys[3], (NUM_HEADS, HEAD_DIM, HIDDEN), jnp.float32) * ((NUM_HEADS * HEAD_DIM) ** -0.5)
    w_up = jax.random.normal(weight_keys[4], (HIDDEN, FFN_DIM), jnp.float32) * (HIDDEN ** -0.5)
    w_down = jax.random.normal(weight_keys[5], (FFN_DIM, HIDDEN), jnp.float32) * (FFN_DIM ** -0.5)
    return {
        "act_x": act_x.astype(jnp.bfloat16),
        "seg_ids": seg_ids,
        "gain_one": gain_one.astype(jnp.bfloat16),
        "gain_two": gain_two.astype(jnp.bfloat16),
        "w_qkv": w_qkv.astype(jnp.bfloat16),
        "w_out": w_out.astype(jnp.bfloat16),
        "w_up": w_up.astype(jnp.bfloat16),
        "w_down": w_down.astype(jnp.bfloat16),
        "grad_y": grad_y.astype(jnp.bfloat16),
    }


def reference(act_x, seg_ids, gain_one, gain_two, w_qkv, w_out, w_up, w_down, grad_y):
    positions = jnp.arange(SEQ_LEN, dtype=jnp.int32)
    allowed = (positions[:, None] >= positions[None, :]) & (seg_ids[:, None] == seg_ids[None, :])

    def one_head(head_rows):
        q_head, k_head, v_head = head_rows
        scores = matmul_f32(q_head, k_head.T) * (HEAD_DIM ** -0.5)
        scores = jnp.where(allowed, scores, -1e30)
        prob_f32 = jax.nn.softmax(scores, axis=-1)
        return matmul_f32(prob_f32.astype(jnp.bfloat16), v_head).astype(jnp.bfloat16)

    head_fn = jax.checkpoint(one_head)

    def layer_map(x_in, g_one, g_two, wqkv_in, wout_in, wup_in, wdown_in):
        normed_one = layer_norm(x_in, g_one).astype(jnp.bfloat16)
        qkv_rows = matmul_f32(normed_one, wqkv_in).astype(jnp.bfloat16)
        qkv_heads = jnp.transpose(qkv_rows.reshape(SEQ_LEN, NUM_HEADS, 3, HEAD_DIM), (2, 1, 0, 3))
        attn_heads = lax.map(head_fn, (qkv_heads[0], qkv_heads[1], qkv_heads[2]))
        attn_rows = jnp.transpose(attn_heads, (1, 0, 2)).reshape(SEQ_LEN, NUM_HEADS * HEAD_DIM)
        attn_proj = matmul_f32(attn_rows, wout_in.reshape(NUM_HEADS * HEAD_DIM, HIDDEN))
        resid_rows = (x_in.astype(jnp.float32) + attn_proj).astype(jnp.bfloat16)
        normed_two = layer_norm(resid_rows, g_two).astype(jnp.bfloat16)
        hidden = jax.nn.gelu(matmul_f32(normed_two, wup_in), approximate=True).astype(jnp.bfloat16)
        return (resid_rows.astype(jnp.float32) + matmul_f32(hidden, wdown_in)).astype(jnp.bfloat16)

    layer_out, pullback = jax.vjp(layer_map, act_x, gain_one, gain_two, w_qkv, w_out, w_up, w_down)
    grads = pullback(grad_y)
    return (layer_out, grads[0], grads[3], grads[4], grads[5], grads[6], grads[1], grads[2])
```

```python
import functools
import jax
import jax.numpy as jnp
from jax import lax
from jax.experimental import pallas as pl
from jax.experimental.pallas import tpu as pltpu
from jax.sharding import PartitionSpec as P

LN_EPS = 1e-5
TILE = 256
BF = jnp.bfloat16
F32 = jnp.float32
gelu_tanh = functools.partial(jax.nn.gelu, approximate=True)


def mm(spec, left, right):
    return jnp.einsum(spec, left, right, preferred_element_type=F32)


def normalize(values):
    values_f32 = values.astype(F32)
    centered = values_f32 - jnp.mean(values_f32, axis=-1, keepdims=True)
    inv_std = lax.rsqrt(jnp.mean(centered * centered, axis=-1, keepdims=True) + LN_EPS)
    return centered * inv_std, inv_std


def norm_backward(grad_out, x_hat, inv_std, gain_vec):
    d_gain = jnp.sum(grad_out * x_hat, axis=0)
    d_hat = grad_out * gain_vec.astype(F32)
    d_in = inv_std * (d_hat - jnp.mean(d_hat, axis=-1, keepdims=True)
                      - x_hat * jnp.mean(d_hat * x_hat, axis=-1, keepdims=True))
    return d_in, d_gain


def dot_nt(left, right):
    return lax.dot_general(left, right, (((1,), (1,)), ((), ())), preferred_element_type=F32)


def dot_tn(left, right):
    return lax.dot_general(left, right, (((0,), (0,)), ((), ())), preferred_element_type=F32)


def dot_nn(left, right):
    return lax.dot_general(left, right, (((1,), (0,)), ((), ())), preferred_element_type=F32)


def scores_t(keys, query, segk_ref, segq, k_start, diagonal):
    block = dot_nt(keys, query) * (query.shape[-1] ** -0.5)
    seen = segk_ref[k_start:k_start + TILE, :] == segq
    if diagonal:
        seen = seen & (lax.broadcasted_iota(jnp.int32, (TILE, TILE), 0)
                       <= lax.broadcasted_iota(jnp.int32, (TILE, TILE), 1))
    return jnp.where(seen, block, -1e30)


def key_blocks(prev, cur, rows, tile, first, dim, part):
    out = []
    for c, ref in enumerate(prev):
        out += [(ref, r, c * rows + r) for r in range(0, rows, TILE)]
    out += [(cur, r, first + r) for r in range(0, (tile + 1) * TILE, TILE)]
    return out


def attn_fwd_kernel(n_prev, rows, dim, *refs):
    segk_ref, segq_ref = refs[:2]
    prev, cur = refs[2:2 + n_prev], refs[2 + n_prev]
    o_ref, stat_ref, s_ref, p_ref = refs[3 + n_prev:]
    first = n_prev * rows
    for t in range(rows // TILE):
        lo = t * TILE
        query = cur[lo:lo + TILE, 0:dim]
        segq = segq_ref[:, first + lo:first + lo + TILE]
        blocks = key_blocks(prev, cur, rows, t, first, dim, 1)
        top = None
        for n, (ref, r, start) in enumerate(blocks):
            block = scores_t(ref[r:r + TILE, dim:2 * dim], query, segk_ref, segq, start, n == len(blocks) - 1)
            s_ref[n * TILE:(n + 1) * TILE, :] = block
            here = jnp.max(block, axis=0, keepdims=True)
            top = here if top is None else jnp.maximum(top, here)
        total = None
        for n in range(len(blocks)):
            expd = jnp.exp(s_ref[n * TILE:(n + 1) * TILE, :] - top)
            s_ref[n * TILE:(n + 1) * TILE, :] = expd
            here = jnp.sum(expd, axis=0, keepdims=True)
            total = here if total is None else total + here
        inv = 1.0 / total
        for n in range(len(blocks)):
            p_ref[n * TILE:(n + 1) * TILE, :] = (s_ref[n * TILE:(n + 1) * TILE, :] * inv).astype(BF)
        out_t = dot_tn(cur[0:lo + TILE, 2 * dim:3 * dim], p_ref[first:first + lo + TILE, :])
        for c, ref in enumerate(prev):
            out_t = out_t + dot_tn(ref[:, 2 * dim:3 * dim], p_ref[c * rows:(c + 1) * rows, :])
        o_ref[lo:lo + TILE, :] = out_t.T.astype(BF)
        stat_ref[0, 0:1, lo:lo + TILE] = top
        stat_ref[0, 1:2, lo:lo + TILE] = inv


def attn_bwd_kernel(n_prev, n_later, rows, dim, *refs):
    segk_ref, segq_ref = refs[:2]
    prev, cur = refs[2:2 + n_prev], refs[2 + n_prev]
    do_ref, stat_ref = refs[3 + n_prev:5 + n_prev]
    later = refs[5 + n_prev:5 + n_prev + n_later]
    rest = refs[5 + n_prev + n_later:]
    dqkv_ref, dkv_prev = rest[0], rest[1:1 + n_prev]
    p_ref, dp_ref, ds_ref, acc_k, acc_v = rest[1 + n_prev:]
    first = n_prev * rows
    scale = dim ** -0.5
    acc_k[...] = jnp.zeros_like(acc_k)
    acc_v[...] = jnp.zeros_like(acc_v)
    for ref in later:
        acc_k[first:first + rows, :] += ref[:, 0:dim]
        acc_v[first:first + rows, :] += ref[:, dim:2 * dim]
    for t in range(rows // TILE):
        lo = t * TILE
        query = cur[lo:lo + TILE, 0:dim]
        d_out = do_ref[lo:lo + TILE, :]
        segq = segq_ref[:, first + lo:first + lo + TILE]
        top = stat_ref[0, 0:1, lo:lo + TILE]
        inv = stat_ref[0, 1:2, lo:lo + TILE]
        blocks = key_blocks(prev, cur, rows, t, first, dim, 1)
        delta = jnp.zeros_like(top)
        for n, (ref, r, start) in enumerate(blocks):
            block = scores_t(ref[r:r + TILE, dim:2 * dim], query, segk_ref, segq, start, n == len(blocks) - 1)
            prob = jnp.exp(block - top) * inv
            d_prob = dot_nt(ref[r:r + TILE, 2 * dim:3 * dim], d_out).astype(BF)
            delta += jnp.sum(prob * d_prob.astype(F32), axis=0, keepdims=True)
            p_ref[n * TILE:(n + 1) * TILE, :] = prob
            dp_ref[n * TILE:(n + 1) * TILE, :] = d_prob
        for n in range(len(blocks)):
            span = slice(n * TILE, (n + 1) * TILE)
            prob = p_ref[span, :]
            d_score = (prob * (dp_ref[span, :].astype(F32) - delta) * scale).astype(BF)
            ds_ref[span, :] = d_score
            acc_v[span, :] += dot_nn(prob.astype(BF), d_out)
            acc_k[span, :] += dot_nn(d_score, query)
        dq_t = dot_tn(cur[0:lo + TILE, dim:2 * dim], ds_ref[first:first + lo + TILE, :])
        for c, ref in enumerate(prev):
            dq_t = dq_t + dot_tn(ref[:, dim:2 * dim], ds_ref[c * rows:(c + 1) * rows, :])
        dqkv_ref[lo:lo + TILE, 0:dim] = dq_t.T.astype(BF)
    dqkv_ref[:, dim:2 * dim] = acc_k[first:first + rows, :].astype(BF)
    dqkv_ref[:, 2 * dim:3 * dim] = acc_v[first:first + rows, :].astype(BF)
    for c, ref in enumerate(dkv_prev):
        ref[:, 0:dim] = acc_k[c * rows:(c + 1) * rows, :]
        ref[:, dim:2 * dim] = acc_v[c * rows:(c + 1) * rows, :]


def whole(shape):
    return pl.BlockSpec(shape, lambda h: (0,) * len(shape))


def by_head(rows, cols):
    return pl.BlockSpec((rows, cols), lambda h: (0, h))


def attn_cost(n_prev, rows, heads, dim, dots):
    area = rows * (n_prev * rows + rows // 2) * heads
    return pl.CostEstimate(flops=2 * area * dim * dots * 2, bytes_accessed=rows * heads * dim * 12, transcendentals=area)


def attention_fwd(segk, segq, qkv_prev, qkv_cur, heads, dim):
    rows, n_prev = qkv_cur.shape[0], len(qkv_prev)
    keys = (n_prev + 1) * rows
    return pl.pallas_call(
        functools.partial(attn_fwd_kernel, n_prev, rows, dim),
        grid=(heads,),
        in_specs=[whole(segk.shape), whole(segq.shape)] + [by_head(rows, 3 * dim)] * (n_prev + 1),
        out_specs=[by_head(rows, dim), pl.BlockSpec((1, 2, rows), lambda h: (h, 0, 0))],
        out_shape=[jax.ShapeDtypeStruct((rows, heads * dim), BF), jax.ShapeDtypeStruct((heads, 2, rows), F32)],
        scratch_shapes=[pltpu.VMEM((keys, TILE), F32), pltpu.VMEM((keys, TILE), BF)],
        cost_estimate=attn_cost(n_prev, rows, heads, dim, 2),
        name=f"attn_fwd_{n_prev}",
    )(segk, segq, *qkv_prev, qkv_cur)


def attention_bwd(segk, segq, qkv_prev, qkv_cur, d_out, stats, later, heads, dim):
    rows, n_prev = qkv_cur.shape[0], len(qkv_prev)
    keys = (n_prev + 1) * rows
    return pl.pallas_call(
        functools.partial(attn_bwd_kernel, n_prev, len(later), rows, dim),
        grid=(heads,),
        in_specs=[whole(segk.shape), whole(segq.shape)] + [by_head(rows, 3 * dim)] * (n_prev + 1)
        + [by_head(rows, dim), pl.BlockSpec((1, 2, rows), lambda h: (h, 0, 0))] + [by_head(rows, 2 * dim)] * len(later),
        out_specs=[by_head(rows, 3 * dim)] + [by_head(rows, 2 * dim)] * n_prev,
        out_shape=[jax.ShapeDtypeStruct((rows, 3 * heads * dim), BF)]
        + [jax.ShapeDtypeStruct((rows, 2 * heads * dim), F32)] * n_prev,
        scratch_shapes=[pltpu.VMEM((keys, TILE), F32), pltpu.VMEM((keys, TILE), BF), pltpu.VMEM((keys, TILE), BF),
                        pltpu.VMEM((keys, dim), F32), pltpu.VMEM((keys, dim), F32)],
        cost_estimate=attn_cost(n_prev, rows, heads, dim, 5),
        name=f"attn_bwd_{n_prev}",
    )(segk, segq, *qkv_prev, qkv_cur, d_out, stats, *later)


def wgrad_kernel(n, *refs):
    out = dot_tn(refs[0][...], refs[n][...])
    for c in range(1, n):
        out += dot_tn(refs[c][...], refs[n + c][...])
    refs[2 * n][...] = out.astype(BF)


def weight_grad(lefts, rights, tile_m, tile_n, name):
    n, rows = len(lefts), lefts[0].shape[0]
    rights = [r if isinstance(r, tuple) else (r, 0) for r in rights]
    m_dim, n_dim = lefts[0].shape[1], rights[0][0].shape[1]
    in_specs = [pl.BlockSpec((rows, tile_m), lambda i, j: (0, i)) for _ in lefts]
    in_specs += [pl.BlockSpec((rows, tile_n), functools.partial(lambda b, i, j: (b, j), b)) for _, b in rights]
    return pl.pallas_call(
        functools.partial(wgrad_kernel, n),
        grid=(m_dim // tile_m, n_dim // tile_n),
        in_specs=in_specs,
        out_specs=pl.BlockSpec((tile_m, tile_n), lambda i, j: (i, j)),
        out_shape=jax.ShapeDtypeStruct((m_dim, n_dim), BF),
        cost_estimate=pl.CostEstimate(flops=2 * n * rows * m_dim * n_dim, transcendentals=0,
                                      bytes_accessed=2 * (n * rows * (m_dim + n_dim) + m_dim * n_dim)),
        compiler_params=pltpu.CompilerParams(vmem_limit_bytes=56 * 1024 * 1024),
        name=name,
    )(*lefts, *[r for r, _ in rights])


def ln_fwd_kernel(x_ref, gain_ref, o_ref):
    hat, _ = normalize(x_ref[...])
    o_ref[...] = (hat * gain_ref[...].astype(F32)).astype(BF)


def ln_mid_kernel(x_ref, sum_ref, gain_ref, x1_ref, o_ref):
    resid = (x_ref[...].astype(F32) + sum_ref[...].astype(F32)).astype(BF)
    x1_ref[...] = resid
    hat, _ = normalize(resid)
    o_ref[...] = (hat * gain_ref[...].astype(F32)).astype(BF)


def ln_bwd_kernel(x_ref, d_ref, gain_ref, resid_ref, o_ref, dg_ref):
    hat, inv_std = normalize(x_ref[...])
    d_in, d_gain = norm_backward(d_ref[...].astype(F32), hat, inv_std, gain_ref[...])
    o_ref[...] = (resid_ref[...].astype(F32) + d_in).astype(BF)
    dg_ref[...] = d_gain[None, :]


def add_kernel(x_ref, sum_ref, o_ref):
    o_ref[...] = (x_ref[...].astype(F32) + sum_ref[...].astype(F32)).astype(BF)


def row_call(kernel, arrays, outs, name, tile=None, start=0):
    rows, width = outs[0][0], arrays[0].shape[1]
    tile = tile or rows
    spec = lambda r, s=0: pl.BlockSpec((r if r == 1 else tile, width), (lambda i: (0, 0)) if r == 1 else (lambda i: (i + s, 0)))
    return pl.pallas_call(
        kernel,
        grid=(rows // tile,),
        in_specs=[spec(a.shape[0], start) for a in arrays],
        out_specs=[spec(r) for r, _ in outs],
        out_shape=[jax.ShapeDtypeStruct((r, width), d) for r, d in outs],
        cost_estimate=pl.CostEstimate(flops=20 * rows * width, bytes_accessed=8 * rows * width, transcendentals=0),
        name=name,
    )(*arrays)


def after(value, *deps):
    return lax.optimization_barrier((value, *deps))[0]


N_CHUNKS = 2


def solution(mesh):
    n_dev = mesh.shape["model"]

    def local_layer(act_x, seg_ids, gain_one, gain_two, w_qkv, w_out, w_up, w_down, grad_y):
        tokens, width = act_x.shape
        heads, dim = w_out.shape[0], w_out.shape[1]
        w_proj = w_out.reshape(heads * dim, width)
        rows = tokens // N_CHUNKS
        own = rows // n_dev
        me = lax.axis_index("model")
        chunks = range(N_CHUNKS)

        def own_rows(array, c):
            return lax.dynamic_slice(array, (c * rows + me * own, 0), (own, array.shape[1]))

        def chunk_of(array, c):
            return array[c * rows:(c + 1) * rows]

        def reduce_rows(part):
            return lax.psum_scatter(part, "model", scatter_dimension=0, tiled=True)

        def gather_rows(block):
            return lax.all_gather(block, "model", axis=0, tiled=True)

        segk = jnp.broadcast_to(seg_ids[:, None], (tokens, TILE))
        segq = seg_ids[None, :]
        gain_one, gain_two = gain_one[None, :], gain_two[None, :]
        last = [seg_ids]

        def turn(value, *deps):
            return after(value, last[0], *deps)

        def done(value):
            last[0] = value
            return value

        def norm_in(c):
            return done(row_call(ln_fwd_kernel, [turn(act_x), gain_one], [(rows, BF)], f"ln1_{c}", 128, c * rows // 128)[0])

        normed_one, qkv, attn, stats, x_own, x1_own, normed_two = [], [], [], [], [], [None] * N_CHUNKS, [None] * N_CHUNKS
        sum_one = []
        for c in chunks:
            normed_one.append(norm_in(c))
            qkv.append(done(mm("sh,hc->sc", turn(normed_one[c]), w_qkv).astype(BF)))
            out, stat = attention_fwd(segk, turn(segq), qkv[:c], qkv[c], heads, dim)
            attn.append(done(out))
            stats.append(stat)
            part = done(mm("sc,ce->se", turn(attn[c]), w_proj).astype(BF))
            sum_one.append(reduce_rows(part))
            x_own.append(own_rows(act_x, c))

        d_hidden = []
        for c in chunks:
            d_hidden.append(done(after(mm("se,fe->sf", chunk_of(turn(grad_y), c), w_down).astype(BF))))
            x1_own[c], block = row_call(ln_mid_kernel, [turn(x_own[c]), sum_one[c], gain_two], [(own, BF)] * 2, f"ln2_{c}")
            normed_two[c] = gather_rows(done(block))

        hidden, d_pre, sum_three = [], [], []
        for c in chunks:
            pre_act = mm("sh,hf->sf", turn(normed_two[c]), w_up)
            act_vals, gelu_pull = jax.vjp(gelu_tanh, pre_act)
            hidden.append(act_vals.astype(BF))
            d_pre.append(done(gelu_pull(d_hidden[c].astype(F32))[0].astype(BF)))
            sum_three.append(reduce_rows(done(mm("sf,hf->sh", turn(d_pre[c]), w_up).astype(BF))))

        part_two = [done(mm("sf,fe->se", turn(hidden[c]), w_down).astype(BF)) for c in chunks]
        d_down = done(weight_grad([turn(hidden[0]), hidden[1]], [(grad_y, c) for c in chunks], 1280, 1280, "d_down"))

        d_resid_own, d_resid, dg_two = [None] * N_CHUNKS, [None] * N_CHUNKS, [None] * N_CHUNKS
        for c in reversed(chunks):
            d_resid_own[c], dg_two[c] = row_call(
                ln_bwd_kernel, [turn(x1_own[c]), sum_three[c], gain_two, own_rows(grad_y, c)], [(own, BF), (1, F32)], f"ln2b_{c}")
            d_resid[c] = gather_rows(done(d_resid_own[c]))

        d_up = done(weight_grad([turn(normed_two[0]), normed_two[1]], d_pre, 1280, 1280, "d_up"))

        d_qkv, later, sum_four, sum_two = [None] * N_CHUNKS, [], [None] * N_CHUNKS, [None] * N_CHUNKS
        for c in reversed(chunks):
            d_attn = done(mm("se,ce->sc", turn(d_resid[c]), w_proj).astype(BF))
            sum_two[c] = reduce_rows(after(part_two[c], d_attn))
            outs = attention_bwd(segk, turn(segq), qkv[:c], qkv[c], d_attn, stats[c], later, heads, dim)
            d_qkv[c], later = done(outs[0]), outs[1:]
            sum_four[c] = reduce_rows(done(mm("sc,hc->sh", turn(d_qkv[c]), w_qkv).astype(BF)))

        y_chunks, x_chunks, dg_one = [None] * N_CHUNKS, [None] * N_CHUNKS, [None] * N_CHUNKS
        for c in reversed(chunks):
            y_own = done(row_call(add_kernel, [turn(x1_own[c]), sum_two[c]], [(own, BF)], f"y_{c}")[0])
            y_chunks[c] = gather_rows(y_own)
            if c == N_CHUNKS - 1:
                d_wout = done(weight_grad([turn(attn[0]), attn[1]], d_resid, heads * dim, 1280, "d_wout"))
            else:
                d_wqkv = done(weight_grad([turn(normed_one[0]), normed_one[1]], d_qkv, 1024, 3 * heads * dim, "d_wqkv"))
            x_new, dg_one[c] = row_call(
                ln_bwd_kernel, [turn(x_own[c]), sum_four[c], gain_one, d_resid_own[c]], [(own, BF), (1, F32)], f"ln1b_{c}")
            x_chunks[c] = gather_rows(done(x_new))

        layer_out = jnp.concatenate(y_chunks, axis=0)
        dg = lax.psum(jnp.concatenate([dg_one[0] + dg_one[1], dg_two[0] + dg_two[1]], axis=0), "model").astype(BF)
        grad_x = jnp.concatenate(x_chunks, axis=0)
        return layer_out, grad_x, d_wqkv, d_wout.reshape(heads, dim, width), d_up, d_down, dg[0], dg[1]

    in_specs = (P("data", None), P("data"), P(None), P(None), P(None, "model"),
                P("model", None, None), P(None, "model"), P("model", None), P("data", None))
    out_specs = (P("data", None), P("data", None), P("data", "model"), P(("data", "model"), None, None),
                 P("data", "model"), P(("data", "model"), None), P("data"), P("data"))
    return jax.shard_map(local_layer, mesh=mesh, in_specs=in_specs, out_specs=out_specs, check_vma=False)
```

```python
import functools
import jax
import jax.numpy as jnp
from jax import lax
from jax.experimental import pallas as pl
from jax.experimental.pallas import tpu as pltpu
from jax.sharding import PartitionSpec as P

LN_EPS = 1e-5
TILE = 256
BF = jnp.bfloat16
F32 = jnp.float32
gelu_tanh = functools.partial(jax.nn.gelu, approximate=True)


def mm(spec, left, right):
    return jnp.einsum(spec, left, right, preferred_element_type=F32)


def normalize(values):
    values_f32 = values.astype(F32)
    centered = values_f32 - jnp.mean(values_f32, axis=-1, keepdims=True)
    inv_std = lax.rsqrt(jnp.mean(centered * centered, axis=-1, keepdims=True) + LN_EPS)
    return centered * inv_std, inv_std


def norm_backward(grad_out, x_hat, inv_std, gain_vec):
    d_gain = jnp.sum(grad_out * x_hat, axis=0)
    d_hat = grad_out * gain_vec.astype(F32)
    d_in = inv_std * (d_hat - jnp.mean(d_hat, axis=-1, keepdims=True)
                      - x_hat * jnp.mean(d_hat * x_hat, axis=-1, keepdims=True))
    return d_in, d_gain


def dot_nt(left, right):
    return lax.dot_general(left, right, (((1,), (1,)), ((), ())), preferred_element_type=F32)


def dot_tn(left, right):
    return lax.dot_general(left, right, (((0,), (0,)), ((), ())), preferred_element_type=F32)


def dot_nn(left, right):
    return lax.dot_general(left, right, (((1,), (0,)), ((), ())), preferred_element_type=F32)


def scores_t(keys, query, segk_ref, segq, k_start, diagonal):
    block = dot_nt(keys, query) * (query.shape[-1] ** -0.5)
    seen = segk_ref[k_start:k_start + TILE, :] == segq
    if diagonal:
        seen = seen & (lax.broadcasted_iota(jnp.int32, (TILE, TILE), 0)
                       <= lax.broadcasted_iota(jnp.int32, (TILE, TILE), 1))
    return jnp.where(seen, block, -1e30)


def key_blocks(prev, cur, rows, tile, first, dim, part):
    out = []
    for c, ref in enumerate(prev):
        out += [(ref, r, c * rows + r) for r in range(0, rows, TILE)]
    out += [(cur, r, first + r) for r in range(0, (tile + 1) * TILE, TILE)]
    return out


def attn_fwd_kernel(n_prev, rows, dim, *refs):
    segk_ref, segq_ref = refs[:2]
    prev, cur = refs[2:2 + n_prev], refs[2 + n_prev]
    o_ref, stat_ref, s_ref, p_ref = refs[3 + n_prev:]
    first = n_prev * rows
    for t in range(rows // TILE):
        lo = t * TILE
        query = cur[lo:lo + TILE, 0:dim]
        segq = segq_ref[:, first + lo:first + lo + TILE]
        blocks = key_blocks(prev, cur, rows, t, first, dim, 1)
        top = None
        for n, (ref, r, start) in enumerate(blocks):
            block = scores_t(ref[r:r + TILE, dim:2 * dim], query, segk_ref, segq, start, n == len(blocks) - 1)
            s_ref[n * TILE:(n + 1) * TILE, :] = block
            here = jnp.max(block, axis=0, keepdims=True)
            top = here if top is None else jnp.maximum(top, here)
        total = None
        for n in range(len(blocks)):
            expd = jnp.exp(s_ref[n * TILE:(n + 1) * TILE, :] - top)
            s_ref[n * TILE:(n + 1) * TILE, :] = expd
            here = jnp.sum(expd, axis=0, keepdims=True)
            total = here if total is None else total + here
        inv = 1.0 / total
        for n in range(len(blocks)):
            p_ref[n * TILE:(n + 1) * TILE, :] = (s_ref[n * TILE:(n + 1) * TILE, :] * inv).astype(BF)
        out_t = dot_tn(cur[0:lo + TILE, 2 * dim:3 * dim], p_ref[first:first + lo + TILE, :])
        for c, ref in enumerate(prev):
            out_t = out_t + dot_tn(ref[:, 2 * dim:3 * dim], p_ref[c * rows:(c + 1) * rows, :])
        o_ref[lo:lo + TILE, :] = out_t.T.astype(BF)
        stat_ref[0, 0:1, lo:lo + TILE] = top
        stat_ref[0, 1:2, lo:lo + TILE] = inv


def attn_bwd_kernel(n_prev, n_later, rows, dim, *refs):
    segk_ref, segq_ref = refs[:2]
    prev, cur = refs[2:2 + n_prev], refs[2 + n_prev]
    do_ref, stat_ref = refs[3 + n_prev:5 + n_prev]
    later = refs[5 + n_prev:5 + n_prev + n_later]
    rest = refs[5 + n_prev + n_later:]
    dqkv_ref, dkv_prev = rest[0], rest[1:1 + n_prev]
    p_ref, dp_ref, ds_ref, acc_k, acc_v = rest[1 + n_prev:]
    first = n_prev * rows
    scale = dim ** -0.5
    acc_k[...] = jnp.zeros_like(acc_k)
    acc_v[...] = jnp.zeros_like(acc_v)
    for ref in later:
        acc_k[first:first + rows, :] += ref[:, 0:dim]
        acc_v[first:first + rows, :] += ref[:, dim:2 * dim]
    for t in range(rows // TILE):
        lo = t * TILE
        query = cur[lo:lo + TILE, 0:dim]
        d_out = do_ref[lo:lo + TILE, :]
        segq = segq_ref[:, first + lo:first + lo + TILE]
        top = stat_ref[0, 0:1, lo:lo + TILE]
        inv = stat_ref[0, 1:2, lo:lo + TILE]
        blocks = key_blocks(prev, cur, rows, t, first, dim, 1)
        delta = jnp.zeros_like(top)
        for n, (ref, r, start) in enumerate(blocks):
            block = scores_t(ref[r:r + TILE, dim:2 * dim], query, segk_ref, segq, start, n == len(blocks) - 1)
            prob = jnp.exp(block - top) * inv
            d_prob = dot_nt(ref[r:r + TILE, 2 * dim:3 * dim], d_out).astype(BF)
            delta += jnp.sum(prob * d_prob.astype(F32), axis=0, keepdims=True)
            p_ref[n * TILE:(n + 1) * TILE, :] = prob
            dp_ref[n * TILE:(n + 1) * TILE, :] = d_prob
        for n in range(len(blocks)):
            span = slice(n * TILE, (n + 1) * TILE)
            prob = p_ref[span, :]
            d_score = (prob * (dp_ref[span, :].astype(F32) - delta) * scale).astype(BF)
            ds_ref[span, :] = d_score
            acc_v[span, :] += dot_nn(prob.astype(BF), d_out)
            acc_k[span, :] += dot_nn(d_score, query)
        dq_t = dot_tn(cur[0:lo + TILE, dim:2 * dim], ds_ref[first:first + lo + TILE, :])
        for c, ref in enumerate(prev):
            dq_t = dq_t + dot_tn(ref[:, dim:2 * dim], ds_ref[c * rows:(c + 1) * rows, :])
        dqkv_ref[lo:lo + TILE, 0:dim] = dq_t.T.astype(BF)
    dqkv_ref[:, dim:2 * dim] = acc_k[first:first + rows, :].astype(BF)
    dqkv_ref[:, 2 * dim:3 * dim] = acc_v[first:first + rows, :].astype(BF)
    for c, ref in enumerate(dkv_prev):
        ref[:, 0:dim] = acc_k[c * rows:(c + 1) * rows, :]
        ref[:, dim:2 * dim] = acc_v[c * rows:(c + 1) * rows, :]


def whole(shape):
    return pl.BlockSpec(shape, lambda h: (0,) * len(shape))


def by_head(rows, cols):
    return pl.BlockSpec((rows, cols), lambda h: (0, h))


def attn_cost(n_prev, rows, heads, dim, dots):
    area = rows * (n_prev * rows + rows // 2) * heads
    return pl.CostEstimate(flops=2 * area * dim * dots * 2, bytes_accessed=rows * heads * dim * 12, transcendentals=area)


def attention_fwd(segk, segq, qkv_prev, qkv_cur, heads, dim):
    rows, n_prev = qkv_cur.shape[0], len(qkv_prev)
    keys = (n_prev + 1) * rows
    return pl.pallas_call(
        functools.partial(attn_fwd_kernel, n_prev, rows, dim),
        grid=(heads,),
        in_specs=[whole(segk.shape), whole(segq.shape)] + [by_head(rows, 3 * dim)] * (n_prev + 1),
        out_specs=[by_head(rows, dim), pl.BlockSpec((1, 2, rows), lambda h: (h, 0, 0))],
        out_shape=[jax.ShapeDtypeStruct((rows, heads * dim), BF), jax.ShapeDtypeStruct((heads, 2, rows), F32)],
        scratch_shapes=[pltpu.VMEM((keys, TILE), F32), pltpu.VMEM((keys, TILE), BF)],
        cost_estimate=attn_cost(n_prev, rows, heads, dim, 2),
        name=f"attn_fwd_{n_prev}",
    )(segk, segq, *qkv_prev, qkv_cur)


def attention_bwd(segk, segq, qkv_prev, qkv_cur, d_out, stats, later, heads, dim):
    rows, n_prev = qkv_cur.shape[0], len(qkv_prev)
    keys = (n_prev + 1) * rows
    return pl.pallas_call(
        functools.partial(attn_bwd_kernel, n_prev, len(later), rows, dim),
        grid=(heads,),
        in_specs=[whole(segk.shape), whole(segq.shape)] + [by_head(rows, 3 * dim)] * (n_prev + 1)
        + [by_head(rows, dim), pl.BlockSpec((1, 2, rows), lambda h: (h, 0, 0))] + [by_head(rows, 2 * dim)] * len(later),
        out_specs=[by_head(rows, 3 * dim)] + [by_head(rows, 2 * dim)] * n_prev,
        out_shape=[jax.ShapeDtypeStruct((rows, 3 * heads * dim), BF)]
        + [jax.ShapeDtypeStruct((rows, 2 * heads * dim), F32)] * n_prev,
        scratch_shapes=[pltpu.VMEM((keys, TILE), F32), pltpu.VMEM((keys, TILE), BF), pltpu.VMEM((keys, TILE), BF),
                        pltpu.VMEM((keys, dim), F32), pltpu.VMEM((keys, dim), F32)],
        cost_estimate=attn_cost(n_prev, rows, heads, dim, 5),
        name=f"attn_bwd_{n_prev}",
    )(segk, segq, *qkv_prev, qkv_cur, d_out, stats, *later)


def wgrad_kernel(n, *refs):
    out = dot_tn(refs[0][...], refs[n][...])
    for c in range(1, n):
        out += dot_tn(refs[c][...], refs[n + c][...])
    refs[2 * n][...] = out.astype(BF)


def weight_grad(lefts, rights, tile_m, tile_n, name):
    n, rows = len(lefts), lefts[0].shape[0]
    rights = [r if isinstance(r, tuple) else (r, 0) for r in rights]
    m_dim, n_dim = lefts[0].shape[1], rights[0][0].shape[1]
    in_specs = [pl.BlockSpec((rows, tile_m), lambda i, j: (0, i)) for _ in lefts]
    in_specs += [pl.BlockSpec((rows, tile_n), functools.partial(lambda b, i, j: (b, j), b)) for _, b in rights]
    return pl.pallas_call(
        functools.partial(wgrad_kernel, n),
        grid=(m_dim // tile_m, n_dim // tile_n),
        in_specs=in_specs,
        out_specs=pl.BlockSpec((tile_m, tile_n), lambda i, j: (i, j)),
        out_shape=jax.ShapeDtypeStruct((m_dim, n_dim), BF),
        cost_estimate=pl.CostEstimate(flops=2 * n * rows * m_dim * n_dim, transcendentals=0,
                                      bytes_accessed=2 * (n * rows * (m_dim + n_dim) + m_dim * n_dim)),
        compiler_params=pltpu.CompilerParams(vmem_limit_bytes=56 * 1024 * 1024),
        name=name,
    )(*lefts, *[r for r, _ in rights])


def ln_mid_kernel(x_ref, keep_ref, got_ref, gain_ref, x1_ref, o_ref):
    resid = (x_ref[...].astype(F32) + (keep_ref[...].astype(F32) + got_ref[...].astype(F32))).astype(BF)
    x1_ref[...] = resid
    hat, _ = normalize(resid)
    o_ref[...] = (hat * gain_ref[...].astype(F32)).astype(BF)


def ln_bwd_kernel(x_ref, keep_ref, got_ref, gain_ref, resid_ref, o_ref, dg_ref):
    hat, inv_std = normalize(x_ref[...])
    d_normed = (keep_ref[...].astype(F32) + got_ref[...].astype(F32)).astype(BF).astype(F32)
    d_in, d_gain = norm_backward(d_normed, hat, inv_std, gain_ref[...])
    o_ref[...] = (resid_ref[...].astype(F32) + d_in).astype(BF)
    dg_ref[...] = d_gain[None, :]


def add_kernel(x_ref, keep_ref, got_ref, o_ref):
    o_ref[...] = (x_ref[...].astype(F32) + (keep_ref[...].astype(F32) + got_ref[...].astype(F32))).astype(BF)


def fold_kernel(own, order_ref, part_ref, got_ref, send_ref, keep_ref):
    for p in range(4):
        src = pl.ds(pl.multiple_of(order_ref[p] * own, 16), own)
        total = (part_ref[src, :].astype(F32) + got_ref[src, :].astype(F32)).astype(BF)
        (send_ref if p < 2 else keep_ref)[(p % 2) * own:(p % 2 + 1) * own, :] = total


def halve_kernel(own, keep_ref, got_ref, send_ref, last_ref):
    total = (keep_ref[...].astype(F32) + got_ref[...].astype(F32)).astype(BF)
    send_ref[...] = total[:own]
    last_ref[...] = total[own:]


def build_kernel(own, start, n, pos_ref, *refs):
    blocks, out_ref = refs[:n], refs[-4]
    held, in_sem, out_sem = refs[-3:]
    loads = [pltpu.make_async_copy(blocks[k], held.at[k], in_sem.at[k]) for k in range(n)]
    for load in loads:
        load.start()
    stores = []
    for k in range(n):
        loads[k].wait()
        spot = out_ref.at[pl.ds(pl.multiple_of(start + pos_ref[k] * own, 16), own), :]
        stores.append(pltpu.make_async_copy(held.at[k], spot, out_sem.at[k]))
        stores[k].start()
    for store in stores:
        store.wait()


def col_call(kernel, head, arrays, out_rows, name, tile=1280):
    width = arrays[0].shape[1]
    spec = lambda r: pl.BlockSpec((r, tile), lambda i: (0, i))
    return pl.pallas_call(
        kernel,
        grid=(width // tile,),
        in_specs=[pl.BlockSpec(memory_space=pltpu.SMEM)] * len(head) + [spec(a.shape[0]) for a in arrays],
        out_specs=[spec(r) for r in out_rows],
        out_shape=[jax.ShapeDtypeStruct((r, width), BF) for r in out_rows],
        cost_estimate=pl.CostEstimate(flops=4 * arrays[0].size, bytes_accessed=6 * arrays[0].size, transcendentals=0),
        name=name,
    )(*head, *arrays)


def build(pos, blocks, start, total, into, name):
    (own, width), n = blocks[0].shape, len(blocks)
    hbm = pl.BlockSpec(memory_space=pl.ANY)
    return pl.pallas_call(
        functools.partial(build_kernel, own, start, n),
        in_specs=[pl.BlockSpec(memory_space=pltpu.SMEM)] + [hbm] * (n + len(into)),
        out_specs=hbm,
        out_shape=jax.ShapeDtypeStruct((total, width), BF),
        scratch_shapes=[pltpu.VMEM((n, own, width), BF), pltpu.SemaphoreType.DMA((n,)), pltpu.SemaphoreType.DMA((n,))],
        input_output_aliases={n + 1: 0} if into else {},
        cost_estimate=pl.CostEstimate(flops=n * own * width, bytes_accessed=4 * n * own * width, transcendentals=0),
        name=name,
    )(pos, *blocks, *into)


def row_call(kernel, arrays, outs, name, tile=None, start=0):
    rows, width = outs[0][0], arrays[0].shape[1]
    tile = tile or rows
    spec = lambda r, s=0: pl.BlockSpec((r if r == 1 else tile, width), (lambda i: (0, 0)) if r == 1 else (lambda i: (i + s, 0)))
    return pl.pallas_call(
        kernel,
        grid=(rows // tile,),
        in_specs=[spec(a.shape[0], start) for a in arrays],
        out_specs=[spec(r) for r, _ in outs],
        out_shape=[jax.ShapeDtypeStruct((r, width), d) for r, d in outs],
        cost_estimate=pl.CostEstimate(flops=20 * rows * width, bytes_accessed=8 * rows * width, transcendentals=0),
        name=name,
    )(*arrays)


def after(value, *deps):
    return lax.optimization_barrier((value, *deps))[0]


N_CHUNKS = 2


def solution(mesh):
    n_dev = mesh.shape["model"]

    def local_layer(act_x, seg_ids, gain_one, gain_two, w_qkv, w_out, w_up, w_down, grad_y):
        tokens, width = act_x.shape
        heads, dim = w_out.shape[0], w_out.shape[1]
        w_proj = w_out.reshape(heads * dim, width)
        rows = tokens // N_CHUNKS
        own = rows // n_dev
        me = lax.axis_index("model")
        chunks = range(N_CHUNKS)

        def own_rows(array, c):
            return lax.dynamic_slice(array, (c * rows + me * own, 0), (own, array.shape[1]))

        def chunk_of(array, c):
            return array[c * rows:(c + 1) * rows]

        core, x_bit, y_bit = me % 2, (me // 2) % 2, me // 4
        swap_core = [(i, i ^ 1) for i in range(n_dev)]
        swap_first = [(i, i ^ (4 if i % 2 else 2)) for i in range(n_dev)]
        swap_second = [(i, i ^ (2 if i % 2 else 4)) for i in range(n_dev)]
        first_step = jnp.where(core == 0, 1, 2)
        here = y_bit * 2 + x_bit
        order = jnp.stack([here ^ 3, here ^ first_step, here ^ (3 - first_step), here]).astype(jnp.int32)

        segk = jnp.broadcast_to(seg_ids[:, None], (tokens, TILE))
        segq = seg_ids[None, :]
        gain_one, gain_two = gain_one[None, :], gain_two[None, :]
        last = [seg_ids]

        def turn(value, *deps):
            return after(value, last[0], *deps)

        def done(value):
            last[0] = value
            return value

        def half_rows(act, which):
            split = act.reshape(n_dev // 2, 2, own, act.shape[1])
            return lax.dynamic_slice_in_dim(split, which, 1, axis=1).reshape(rows // 2, act.shape[1])

        class Reduce:
            def __init__(self, spec, act, weight, name):
                self.name = name
                part = done(mm(spec, half_rows(turn(act), 1 - core), weight).astype(BF))
                self.got = lax.ppermute(part, "model", swap_core)
                self.part = done(mm(spec, half_rows(turn(act), core), weight).astype(BF))

            def fold(self):
                send, self.keep = col_call(functools.partial(fold_kernel, own), [order], [turn(self.part), self.got],
                                           [2 * own, 2 * own], self.name + "_fold")
                done(send)
                self.got = lax.ppermute(send, "model", swap_first)

            def halve(self):
                send, self.keep = col_call(functools.partial(halve_kernel, own), [], [turn(self.keep), self.got],
                                           [own, own], self.name + "_halve")
                done(send)
                self.got = lax.ppermute(send, "model", swap_second)

        places = jnp.stack([me ^ k for k in (0, 2, 4, 6, 1, 3, 5, 7)]).astype(jnp.int32)

        class Gather:
            def __init__(self, block):
                self.block = block
                self.far = [self.send(block, step) for step in (2, 4, 6)]
                self.near = [self.send(block, 1)]

            def send(self, block, step):
                return lax.ppermute(block, "model", [(i, i ^ step) for i in range(n_dev)])

            def cross(self):
                *self.far, _ = lax.optimization_barrier((*self.far, last[0]))
                done(self.far[0])
                self.near += [self.send(block, 1) for block in self.far]

            def build(self, name, start=0, total=rows, into=()):
                blocks = [turn(self.block), *self.far, *self.near]
                return done(build(places, blocks, start, total, list(into), name))

        normed_one, qkv, attn, stats = [None] * 2, [None] * 2, [None] * 2, [None] * 2
        x_own = [own_rows(act_x, c) for c in chunks]
        dy_own = [own_rows(grad_y, c) for c in chunks]
        x1_own, normed_two, d_hidden, hidden, d_pre = [None] * 2, [None] * 2, [None] * 2, [None] * 2, [None] * 2
        d_resid_own, d_resid, d_attn, d_qkv = [None] * 2, [None] * 2, [None] * 2, [None] * 2
        dg_two, dg_one = [None] * 2, [None] * 2

        def do_qkv(c):
            hat, _ = normalize(chunk_of(turn(act_x), c))
            normed_one[c] = done((hat * gain_one.astype(F32)).astype(BF))
            qkv[c] = done(mm("sh,hc->sc", turn(normed_one[c]), w_qkv).astype(BF))

        def do_attn(c):
            out, stats[c] = attention_fwd(segk, turn(segq), qkv[:c], qkv[c], heads, dim)
            attn[c] = done(out)

        def do_d_hidden(c):
            d_hidden[c] = done(after(mm("se,fe->sf", chunk_of(turn(grad_y), c), w_down).astype(BF)))

        def do_mid(c, red):
            x1_own[c], block = row_call(
                ln_mid_kernel, [turn(x_own[c]), red.keep, red.got, gain_two], [(own, BF)] * 2, f"ln2_{c}")
            return Gather(done(block))

        def do_up(c):
            pre_act = mm("sh,hf->sf", turn(normed_two[c]), w_up)
            act_vals, gelu_pull = jax.vjp(gelu_tanh, pre_act)
            hidden[c] = act_vals.astype(BF)
            d_pre[c] = done(gelu_pull(d_hidden[c].astype(F32))[0].astype(BF))

        def do_mid_bwd(c, red):
            d_resid_own[c], dg_two[c] = row_call(
                ln_bwd_kernel, [turn(x1_own[c]), red.keep, red.got, gain_two, dy_own[c]], [(own, BF), (1, F32)], f"ln2b_{c}")
            return Gather(done(d_resid_own[c]))

        def do_attn_bwd(c, later):
            d_attn = done(mm("se,ce->sc", turn(d_resid[c]), w_proj).astype(BF))
            outs = attention_bwd(segk, turn(segq), qkv[:c], qkv[c], d_attn, stats[c], later, heads, dim)
            d_qkv[c] = done(outs[0])
            return outs[1:]

        def do_y(c, red):
            y_own = done(row_call(add_kernel, [turn(x1_own[c]), red.keep, red.got], [(own, BF)], f"y_{c}")[0])
            return Gather(y_own)

        def do_in_bwd(c, red):
            block, dg_one[c] = row_call(
                ln_bwd_kernel, [turn(x_own[c]), red.keep, red.got, gain_one, d_resid_own[c]], [(own, BF), (1, F32)], f"ln1b_{c}")
            return Gather(done(block))

        do_qkv(0)
        do_attn(0)
        one_a = Reduce("sc,ce->se", attn[0], w_proj, "one_a")
        do_qkv(1)
        one_a.fold()
        do_attn(1)
        one_b = Reduce("sc,ce->se", attn[1], w_proj, "one_b")
        one_a.halve()
        one_b.fold()
        do_d_hidden(0)
        mid_a = do_mid(0, one_a)
        one_b.halve()
        do_d_hidden(1)
        mid_b = do_mid(1, one_b)
        mid_a.cross()
        normed_two[0] = mid_a.build("mid_a")
        do_up(0)
        three_a = Reduce("sf,hf->sh", d_pre[0], w_up, "three_a")
        mid_b.cross()
        three_a.fold()
        normed_two[1] = mid_b.build("mid_b")
        do_up(1)
        three_a.halve()
        three_b = Reduce("sf,hf->sh", d_pre[1], w_up, "three_b")
        three_b.fold()
        res_a = do_mid_bwd(0, three_a)
        two_a = Reduce("sf,fe->se", hidden[0], w_down, "two_a")
        three_b.halve()
        two_b = Reduce("sf,fe->se", hidden[1], w_down, "two_b")
        res_b = do_mid_bwd(1, three_b)
        two_a.fold()
        res_a.cross()
        d_down = done(weight_grad([turn(hidden[0]), hidden[1]], [(grad_y, c) for c in chunks], 1280, 1280, "d_down"))
        two_b.fold()
        res_b.cross()
        d_resid[0] = res_a.build("res_a")
        d_resid[1] = res_b.build("res_b")
        later = do_attn_bwd(1, [])
        two_a.halve()
        four_b = Reduce("sc,hc->sh", d_qkv[1], w_qkv, "four_b")
        two_b.halve()
        four_b.fold()
        y_a = do_y(0, two_a)
        do_attn_bwd(0, later)
        y_b = do_y(1, two_b)
        four_b.halve()
        four_a = Reduce("sc,hc->sh", d_qkv[0], w_qkv, "four_a")
        y_a.cross()
        four_a.fold()
        x_b = do_in_bwd(1, four_b)
        layer_out = y_a.build("y_a", 0, tokens)
        d_up = done(weight_grad([turn(normed_two[0]), normed_two[1]], d_pre, 1280, 1280, "d_up"))
        four_a.halve()
        y_b.cross()
        d_wout = done(weight_grad([turn(attn[0]), attn[1]], d_resid, heads * dim, 1280, "d_wout"))
        x_a = do_in_bwd(0, four_a)
        x_b.cross()
        dg = jnp.concatenate([dg_one[0] + dg_one[1], dg_two[0] + dg_two[1]], axis=0)
        layer_out = y_b.build("y_b", rows, tokens, [layer_out])
        d_wqkv = done(weight_grad([turn(normed_one[0]), normed_one[1]], d_qkv, 1024, 3 * heads * dim, "d_wqkv"))
        x_a.cross()
        for step in (1, 2, 4):
            dg = dg + lax.ppermute(dg, "model", [(i, i ^ step) for i in range(n_dev)])
        grad_x = x_b.build("x_b", rows, tokens)
        grad_x = x_a.build("x_a", 0, tokens, [grad_x])
        dg = dg.astype(BF)
        return layer_out, grad_x, d_wqkv, d_wout.reshape(heads, dim, width), d_up, d_down, dg[0], dg[1]

    in_specs = (P("data", None), P("data"), P(None), P(None), P(None, "model"),
                P("model", None, None), P(None, "model"), P("model", None), P("data", None))
    out_specs = (P("data", None), P("data", None), P("data", "model"), P(("data", "model"), None, None),
                 P("data", "model"), P(("data", "model"), None), P("data"), P("data"))
    return jax.shard_map(local_layer, mesh=mesh, in_specs=in_specs, out_specs=out_specs, check_vma=False)
```

```python
import functools
import jax
import jax.numpy as jnp
from jax import lax
from jax.experimental import pallas as pl
from jax.experimental.pallas import tpu as pltpu
from jax.sharding import PartitionSpec as P

LN_EPS = 1e-5
TILE = 256
BF = jnp.bfloat16
F32 = jnp.float32
gelu_tanh = functools.partial(jax.nn.gelu, approximate=True)


def mm(spec, left, right):
    return jnp.einsum(spec, left, right, preferred_element_type=F32)


def normalize(values):
    values_f32 = values.astype(F32)
    centered = values_f32 - jnp.mean(values_f32, axis=-1, keepdims=True)
    inv_std = lax.rsqrt(jnp.mean(centered * centered, axis=-1, keepdims=True) + LN_EPS)
    return centered * inv_std, inv_std


def norm_backward(grad_out, x_hat, inv_std, gain_vec):
    d_gain = jnp.sum(grad_out * x_hat, axis=0)
    d_hat = grad_out * gain_vec.astype(F32)
    d_in = inv_std * (d_hat - jnp.mean(d_hat, axis=-1, keepdims=True)
                      - x_hat * jnp.mean(d_hat * x_hat, axis=-1, keepdims=True))
    return d_in, d_gain


def dot_nt(left, right):
    return lax.dot_general(left, right, (((1,), (1,)), ((), ())), preferred_element_type=F32)


def dot_tn(left, right):
    return lax.dot_general(left, right, (((0,), (0,)), ((), ())), preferred_element_type=F32)


def dot_nn(left, right):
    return lax.dot_general(left, right, (((1,), (0,)), ((), ())), preferred_element_type=F32)


def scores_t(keys, query, segk_ref, segq, k_start, diagonal):
    block = dot_nt(keys, query) * (query.shape[-1] ** -0.5)
    seen = segk_ref[k_start:k_start + TILE, :] == segq
    if diagonal:
        seen = seen & (lax.broadcasted_iota(jnp.int32, (TILE, TILE), 0)
                       <= lax.broadcasted_iota(jnp.int32, (TILE, TILE), 1))
    return jnp.where(seen, block, -1e30)


def key_blocks(prev, cur, rows, tile, first, dim, part):
    out = []
    for c, ref in enumerate(prev):
        out += [(ref, r, c * rows + r) for r in range(0, rows, TILE)]
    out += [(cur, r, first + r) for r in range(0, (tile + 1) * TILE, TILE)]
    return out


def attn_fwd_kernel(n_prev, rows, dim, *refs):
    segk_ref, segq_ref = refs[:2]
    prev, cur = refs[2:2 + n_prev], refs[2 + n_prev]
    o_ref, stat_ref, s_ref, p_ref = refs[3 + n_prev:]
    first = n_prev * rows
    for t in range(rows // TILE):
        lo = t * TILE
        query = cur[lo:lo + TILE, 0:dim]
        segq = segq_ref[:, first + lo:first + lo + TILE]
        blocks = key_blocks(prev, cur, rows, t, first, dim, 1)
        top = None
        for n, (ref, r, start) in enumerate(blocks):
            block = scores_t(ref[r:r + TILE, dim:2 * dim], query, segk_ref, segq, start, n == len(blocks) - 1)
            s_ref[n * TILE:(n + 1) * TILE, :] = block
            here = jnp.max(block, axis=0, keepdims=True)
            top = here if top is None else jnp.maximum(top, here)
        total = None
        for n in range(len(blocks)):
            expd = jnp.exp(s_ref[n * TILE:(n + 1) * TILE, :] - top)
            s_ref[n * TILE:(n + 1) * TILE, :] = expd
            here = jnp.sum(expd, axis=0, keepdims=True)
            total = here if total is None else total + here
        inv = 1.0 / total
        for n in range(len(blocks)):
            p_ref[n * TILE:(n + 1) * TILE, :] = (s_ref[n * TILE:(n + 1) * TILE, :] * inv).astype(BF)
        out_t = dot_tn(cur[0:lo + TILE, 2 * dim:3 * dim], p_ref[first:first + lo + TILE, :])
        for c, ref in enumerate(prev):
            out_t = out_t + dot_tn(ref[:, 2 * dim:3 * dim], p_ref[c * rows:(c + 1) * rows, :])
        o_ref[lo:lo + TILE, :] = out_t.T.astype(BF)
        stat_ref[0, 0:1, lo:lo + TILE] = top
        stat_ref[0, 1:2, lo:lo + TILE] = inv


def attn_bwd_kernel(n_prev, n_later, rows, dim, *refs):
    segk_ref, segq_ref = refs[:2]
    prev, cur = refs[2:2 + n_prev], refs[2 + n_prev]
    do_ref, stat_ref = refs[3 + n_prev:5 + n_prev]
    later = refs[5 + n_prev:5 + n_prev + n_later]
    rest = refs[5 + n_prev + n_later:]
    dqkv_ref, dkv_prev = rest[0], rest[1:1 + n_prev]
    p_ref, dp_ref, ds_ref, acc_k, acc_v = rest[1 + n_prev:]
    first = n_prev * rows
    scale = dim ** -0.5
    acc_k[...] = jnp.zeros_like(acc_k)
    acc_v[...] = jnp.zeros_like(acc_v)
    for ref in later:
        acc_k[first:first + rows, :] += ref[:, 0:dim]
        acc_v[first:first + rows, :] += ref[:, dim:2 * dim]
    for t in range(rows // TILE):
        lo = t * TILE
        query = cur[lo:lo + TILE, 0:dim]
        d_out = do_ref[lo:lo + TILE, :]
        segq = segq_ref[:, first + lo:first + lo + TILE]
        top = stat_ref[0, 0:1, lo:lo + TILE]
        inv = stat_ref[0, 1:2, lo:lo + TILE]
        blocks = key_blocks(prev, cur, rows, t, first, dim, 1)
        delta = jnp.zeros_like(top)
        for n, (ref, r, start) in enumerate(blocks):
            block = scores_t(ref[r:r + TILE, dim:2 * dim], query, segk_ref, segq, start, n == len(blocks) - 1)
            prob = jnp.exp(block - top) * inv
            d_prob = dot_nt(ref[r:r + TILE, 2 * dim:3 * dim], d_out).astype(BF)
            delta += jnp.sum(prob * d_prob.astype(F32), axis=0, keepdims=True)
            p_ref[n * TILE:(n + 1) * TILE, :] = prob
            dp_ref[n * TILE:(n + 1) * TILE, :] = d_prob
        for n in range(len(blocks)):
            span = slice(n * TILE, (n + 1) * TILE)
            prob = p_ref[span, :]
            d_score = (prob * (dp_ref[span, :].astype(F32) - delta) * scale).astype(BF)
            ds_ref[span, :] = d_score
            acc_v[span, :] += dot_nn(prob.astype(BF), d_out)
            acc_k[span, :] += dot_nn(d_score, query)
        dq_t = dot_tn(cur[0:lo + TILE, dim:2 * dim], ds_ref[first:first + lo + TILE, :])
        for c, ref in enumerate(prev):
            dq_t = dq_t + dot_tn(ref[:, dim:2 * dim], ds_ref[c * rows:(c + 1) * rows, :])
        dqkv_ref[lo:lo + TILE, 0:dim] = dq_t.T.astype(BF)
    dqkv_ref[:, dim:2 * dim] = acc_k[first:first + rows, :].astype(BF)
    dqkv_ref[:, 2 * dim:3 * dim] = acc_v[first:first + rows, :].astype(BF)
    for c, ref in enumerate(dkv_prev):
        ref[:, 0:dim] = acc_k[c * rows:(c + 1) * rows, :]
        ref[:, dim:2 * dim] = acc_v[c * rows:(c + 1) * rows, :]


def whole(shape):
    return pl.BlockSpec(shape, lambda h: (0,) * len(shape))


def by_head(rows, cols):
    return pl.BlockSpec((rows, cols), lambda h: (0, h))


def attn_cost(n_prev, rows, heads, dim, dots):
    area = rows * (n_prev * rows + rows // 2) * heads
    return pl.CostEstimate(flops=2 * area * dim * dots * 2, bytes_accessed=rows * heads * dim * 12, transcendentals=area)


def attention_fwd(segk, segq, qkv_prev, qkv_cur, heads, dim):
    rows, n_prev = qkv_cur.shape[0], len(qkv_prev)
    keys = (n_prev + 1) * rows
    return pl.pallas_call(
        functools.partial(attn_fwd_kernel, n_prev, rows, dim),
        grid=(heads,),
        in_specs=[whole(segk.shape), whole(segq.shape)] + [by_head(rows, 3 * dim)] * (n_prev + 1),
        out_specs=[by_head(rows, dim), pl.BlockSpec((1, 2, rows), lambda h: (h, 0, 0))],
        out_shape=[jax.ShapeDtypeStruct((rows, heads * dim), BF), jax.ShapeDtypeStruct((heads, 2, rows), F32)],
        scratch_shapes=[pltpu.VMEM((keys, TILE), F32), pltpu.VMEM((keys, TILE), BF)],
        cost_estimate=attn_cost(n_prev, rows, heads, dim, 2),
        name=f"attn_fwd_{n_prev}",
    )(segk, segq, *qkv_prev, qkv_cur)


def attention_bwd(segk, segq, qkv_prev, qkv_cur, d_out, stats, later, heads, dim):
    rows, n_prev = qkv_cur.shape[0], len(qkv_prev)
    keys = (n_prev + 1) * rows
    return pl.pallas_call(
        functools.partial(attn_bwd_kernel, n_prev, len(later), rows, dim),
        grid=(heads,),
        in_specs=[whole(segk.shape), whole(segq.shape)] + [by_head(rows, 3 * dim)] * (n_prev + 1)
        + [by_head(rows, dim), pl.BlockSpec((1, 2, rows), lambda h: (h, 0, 0))] + [by_head(rows, 2 * dim)] * len(later),
        out_specs=[by_head(rows, 3 * dim)] + [by_head(rows, 2 * dim)] * n_prev,
        out_shape=[jax.ShapeDtypeStruct((rows, 3 * heads * dim), BF)]
        + [jax.ShapeDtypeStruct((rows, 2 * heads * dim), F32)] * n_prev,
        scratch_shapes=[pltpu.VMEM((keys, TILE), F32), pltpu.VMEM((keys, TILE), BF), pltpu.VMEM((keys, TILE), BF),
                        pltpu.VMEM((keys, dim), F32), pltpu.VMEM((keys, dim), F32)],
        cost_estimate=attn_cost(n_prev, rows, heads, dim, 5),
        name=f"attn_bwd_{n_prev}",
    )(segk, segq, *qkv_prev, qkv_cur, d_out, stats, *later)


def wgrad_kernel(n, *refs):
    out = dot_tn(refs[0][...], refs[n][...])
    for c in range(1, n):
        out += dot_tn(refs[c][...], refs[n + c][...])
    refs[-1][...] = out.astype(BF)


def weight_grad(lefts, rights, tile_m, tile_n, name, first=0, count=None, into=()):
    n, rows = len(lefts), lefts[0].shape[0]
    rights = [r if isinstance(r, tuple) else (r, 0) for r in rights]
    m_dim, n_dim = lefts[0].shape[1], rights[0][0].shape[1]
    count = count or m_dim // tile_m - first
    part = count * tile_m
    in_specs = [pl.BlockSpec((rows, tile_m), lambda i, j: (0, i + first)) for _ in lefts]
    in_specs += [pl.BlockSpec((rows, tile_n), functools.partial(lambda b, i, j: (b, j), b)) for _, b in rights]
    return pl.pallas_call(
        functools.partial(wgrad_kernel, n),
        grid=(count, n_dim // tile_n),
        in_specs=in_specs + [pl.BlockSpec(memory_space=pl.ANY)] * len(into),
        out_specs=pl.BlockSpec((tile_m, tile_n), lambda i, j: (i + first, j)),
        out_shape=jax.ShapeDtypeStruct((m_dim, n_dim), BF),
        input_output_aliases={2 * n: 0} if into else {},
        cost_estimate=pl.CostEstimate(flops=2 * n * rows * part * n_dim, transcendentals=0,
                                      bytes_accessed=2 * (n * rows * (part + n_dim) + part * n_dim)),
        compiler_params=pltpu.CompilerParams(vmem_limit_bytes=56 * 1024 * 1024),
        name=name,
    )(*lefts, *[r for r, _ in rights], *into)


def ln_mid_kernel(x_ref, keep_ref, got_ref, gain_ref, x1_ref, o_ref):
    resid = (x_ref[...].astype(F32) + (keep_ref[...].astype(F32) + got_ref[...].astype(F32))).astype(BF)
    x1_ref[...] = resid
    hat, _ = normalize(resid)
    o_ref[...] = (hat * gain_ref[...].astype(F32)).astype(BF)


def ln_bwd_kernel(x_ref, keep_ref, got_ref, gain_ref, resid_ref, o_ref, dg_ref):
    hat, inv_std = normalize(x_ref[...])
    d_normed = (keep_ref[...].astype(F32) + got_ref[...].astype(F32)).astype(BF).astype(F32)
    d_in, d_gain = norm_backward(d_normed, hat, inv_std, gain_ref[...])
    o_ref[...] = (resid_ref[...].astype(F32) + d_in).astype(BF)
    dg_ref[...] = d_gain[None, :]


def add_kernel(x_ref, sum_ref, o_ref):
    o_ref[...] = (x_ref[...].astype(F32) + sum_ref[...].astype(F32)).astype(BF)


def part_kernel(own, transposed, order_ref, act_ref, w_ref, far_ref, near_ref, rows_ref):
    n = act_ref.shape[0] // own

    @pl.when(pl.program_id(0) == 0)
    def _():
        for p in range(n):
            rows_ref[p * own:(p + 1) * own, :] = act_ref[pl.ds(pl.multiple_of(order_ref[p] * own, 16), own), :]

    total = (dot_nt if transposed else dot_nn)(rows_ref[...], w_ref[...]).astype(BF)
    far_ref[...] = total[:n // 2 * own]
    near_ref[...] = total[n // 2 * own:]


def part_call(order, act, weight, own, transposed, name, tile=512):
    rows, depth = act.shape
    width = weight.shape[0 if transposed else 1]
    w_spec = (pl.BlockSpec((tile, depth), lambda i: (i, 0)) if transposed
              else pl.BlockSpec((depth, tile), lambda i: (0, i)))
    half = pl.BlockSpec((rows // 2, tile), lambda i: (0, i))
    return pl.pallas_call(
        functools.partial(part_kernel, own, transposed),
        grid=(width // tile,),
        in_specs=[pl.BlockSpec(memory_space=pltpu.SMEM), pl.BlockSpec((rows, depth), lambda i: (0, 0)), w_spec],
        out_specs=[half, half],
        out_shape=[jax.ShapeDtypeStruct((rows // 2, width), BF)] * 2,
        scratch_shapes=[pltpu.VMEM((rows, depth), BF)],
        cost_estimate=pl.CostEstimate(flops=2 * rows * depth * width, transcendentals=0,
                                      bytes_accessed=2 * (rows * depth + depth * width + rows * width)),
        name=name,
    )(order, act, weight)


def fold_kernel(own, part_ref, got_ref, send_ref, keep_ref):
    total = (part_ref[...].astype(F32) + got_ref[...].astype(F32)).astype(BF)
    send_ref[...] = total[:2 * own]
    keep_ref[...] = total[2 * own:]


def halve_kernel(own, keep_ref, got_ref, send_ref, last_ref):
    total = (keep_ref[...].astype(F32) + got_ref[...].astype(F32)).astype(BF)
    send_ref[...] = total[:own]
    last_ref[...] = total[own:]


def place_kernel(x_ref, *refs):
    refs[-1][...] = x_ref[...]


def col_call(kernel, head, arrays, out_rows, name, tile=640):
    width = arrays[0].shape[1]
    spec = lambda r: pl.BlockSpec((r, tile), lambda i: (0, i))
    return pl.pallas_call(
        kernel,
        grid=(width // tile,),
        in_specs=[pl.BlockSpec(memory_space=pltpu.SMEM)] * len(head) + [spec(a.shape[0]) for a in arrays],
        out_specs=[spec(r) for r in out_rows],
        out_shape=[jax.ShapeDtypeStruct((r, width), BF) for r in out_rows],
        cost_estimate=pl.CostEstimate(flops=4 * arrays[0].size, bytes_accessed=6 * arrays[0].size, transcendentals=0),
        name=name,
    )(*head, *arrays)


def place(block, start, total, into, name, tile=128):
    rows, width = block.shape
    first = start // tile
    return pl.pallas_call(
        place_kernel,
        grid=(rows // tile,),
        in_specs=[pl.BlockSpec((tile, width), lambda i: (i, 0))] + [pl.BlockSpec(memory_space=pl.ANY)] * len(into),
        out_specs=pl.BlockSpec((tile, width), lambda i: (i + first, 0)),
        out_shape=jax.ShapeDtypeStruct((total, width), BF),
        input_output_aliases={1: 0} if into else {},
        cost_estimate=pl.CostEstimate(flops=rows * width, bytes_accessed=4 * rows * width, transcendentals=0),
        name=name,
    )(block, *into)


def row_call(kernel, arrays, outs, name, tile=None, start=0):
    rows, width = outs[0][0], arrays[0].shape[1]
    tile = tile or rows
    spec = lambda r, s=0: pl.BlockSpec((r if r == 1 else tile, width), (lambda i: (0, 0)) if r == 1 else (lambda i: (i + s, 0)))
    return pl.pallas_call(
        kernel,
        grid=(rows // tile,),
        in_specs=[spec(a.shape[0], start) for a in arrays],
        out_specs=[spec(r) for r, _ in outs],
        out_shape=[jax.ShapeDtypeStruct((r, width), d) for r, d in outs],
        cost_estimate=pl.CostEstimate(flops=20 * rows * width, bytes_accessed=8 * rows * width, transcendentals=0),
        name=name,
    )(*arrays)


def after(value, *deps):
    return lax.optimization_barrier((value, *deps))[0]


N_CHUNKS = 2


def solution(mesh):
    n_dev = mesh.shape["model"]

    def local_layer(act_x, seg_ids, gain_one, gain_two, w_qkv, w_out, w_up, w_down, grad_y):
        tokens, width = act_x.shape
        heads, dim = w_out.shape[0], w_out.shape[1]
        w_proj = w_out.reshape(heads * dim, width)
        rows = tokens // N_CHUNKS
        own = rows // n_dev
        me = lax.axis_index("model")
        chunks = range(N_CHUNKS)

        def own_rows(array, c):
            return lax.dynamic_slice(array, (c * rows + me * own, 0), (own, array.shape[1]))

        def chunk_of(array, c):
            return array[c * rows:(c + 1) * rows]

        def gather_rows(block):
            return lax.all_gather(block, "model", axis=0, tiled=True)

        core, x_bit, y_bit = me % 2, (me // 2) % 2, me // 4
        swap_core = [(i, i ^ 1) for i in range(n_dev)]
        swap_first = [(i, i ^ (4 if i % 2 else 2)) for i in range(n_dev)]
        swap_second = [(i, i ^ (2 if i % 2 else 4)) for i in range(n_dev)]
        here = y_bit * 2 + x_bit

        def order_of(which):
            first_step = jnp.where(which == 0, 1, 2)
            return [(here ^ 3) * 2 + which, (here ^ first_step) * 2 + which, (here ^ (3 - first_step)) * 2 + which,
                    here * 2 + which]

        order = jnp.stack(order_of(1 - core) + order_of(core)).astype(jnp.int32)

        segk = jnp.broadcast_to(seg_ids[:, None], (tokens, TILE))
        segq = seg_ids[None, :]
        gain_one, gain_two = gain_one[None, :], gain_two[None, :]
        last = [seg_ids]

        def turn(value, *deps):
            return after(value, last[0], *deps)

        def done(value):
            last[0] = value
            return value

        class Reduce:
            def __init__(self, act, weight, transposed, name):
                self.name = name
                part, self.part = part_call(order, turn(act), weight, own, transposed, name)
                done(part)
                self.got = lax.ppermute(part, "model", swap_core)

            def fold(self):
                send, self.keep = col_call(functools.partial(fold_kernel, own), [], [turn(self.part), self.got],
                                           [2 * own, 2 * own], self.name + "_fold")
                done(send)
                self.got = lax.ppermute(send, "model", swap_first)

            def halve(self):
                send, self.keep = col_call(functools.partial(halve_kernel, own), [], [turn(self.keep), self.got],
                                           [own, own], self.name + "_halve")
                done(send)
                self.got = lax.ppermute(send, "model", swap_second)

        normed_one, qkv, attn, stats = [None] * 2, [None] * 2, [None] * 2, [None] * 2
        x_own = [own_rows(act_x, c) for c in chunks]
        dy_own = [own_rows(grad_y, c) for c in chunks]
        x1_own, normed_two, d_hidden, hidden, d_pre = [None] * 2, [None] * 2, [None] * 2, [None] * 2, [None] * 2
        d_resid_own, d_resid, d_attn, d_qkv = [None] * 2, [None] * 2, [None] * 2, [None] * 2
        dg_two, dg_one, y_full, x_new = [None] * 2, [None] * 2, [None] * 2, [None] * 2

        def do_qkv(c):
            hat, _ = normalize(chunk_of(turn(act_x), c))
            normed_one[c] = done((hat * gain_one.astype(F32)).astype(BF))
            qkv[c] = done(mm("sh,hc->sc", turn(normed_one[c]), w_qkv).astype(BF))

        def do_attn(c):
            out, stats[c] = attention_fwd(segk, turn(segq), qkv[:c], qkv[c], heads, dim)
            attn[c] = done(out)

        def do_d_hidden(c):
            d_hidden[c] = done(after(mm("se,fe->sf", chunk_of(turn(grad_y), c), w_down).astype(BF)))

        def do_mid(c, red):
            x1_own[c], block = row_call(
                ln_mid_kernel, [turn(x_own[c]), red.keep, red.got, gain_two], [(own, BF)] * 2, f"ln2_{c}")
            normed_two[c] = gather_rows(done(block))

        def do_up(c):
            pre_act = mm("sh,hf->sf", turn(normed_two[c]), w_up)
            act_vals, gelu_pull = jax.vjp(gelu_tanh, pre_act)
            hidden[c] = act_vals.astype(BF)
            d_pre[c] = done(gelu_pull(d_hidden[c].astype(F32))[0].astype(BF))

        def do_mid_bwd(c, red):
            d_resid_own[c], dg_two[c] = row_call(
                ln_bwd_kernel, [turn(x1_own[c]), red.keep, red.got, gain_two, dy_own[c]], [(own, BF), (1, F32)], f"ln2b_{c}")
            d_resid[c] = gather_rows(done(d_resid_own[c]))

        def do_attn_bwd(c, later):
            outs = attention_bwd(segk, turn(segq), qkv[:c], qkv[c], d_attn[c], stats[c], later, heads, dim)
            d_qkv[c] = done(outs[0])
            return outs[1:]

        def do_y(c, red):
            y_own = done(row_call(add_kernel, [turn(x1_own[c]), red], [(own, BF)], f"y_{c}")[0])
            y_full[c] = gather_rows(y_own)

        def do_in_bwd(c, red):
            block, dg_one[c] = row_call(
                ln_bwd_kernel, [turn(x_own[c]), red.keep, red.got, gain_one, d_resid_own[c]], [(own, BF), (1, F32)], f"ln1b_{c}")
            x_new[c] = gather_rows(done(block))

        def do_down(c):
            return done(mm("sf,fe->se", turn(hidden[c]), w_down).astype(BF))

        def scatter(part):
            return lax.psum_scatter(part, "model", scatter_dimension=0, tiled=True)

        do_qkv(0)
        do_attn(0)
        one_a = Reduce(attn[0], w_proj, False, "one_a")
        hat, _ = normalize(chunk_of(turn(act_x), 1))
        normed_one[1] = done((hat * gain_one.astype(F32)).astype(BF))
        one_a.fold()
        qkv[1] = done(mm("sh,hc->sc", turn(normed_one[1]), w_qkv).astype(BF))
        one_a.halve()
        do_attn(1)
        do_mid(0, one_a)
        one_b = Reduce(attn[1], w_proj, False, "one_b")
        do_d_hidden(0)
        one_b.fold()
        do_d_hidden(1)
        one_b.halve()
        do_up(0)
        do_mid(1, one_b)
        three_a = Reduce(d_pre[0], w_up, True, "three_a")
        two_a = do_down(0)
        sum_two_a = scatter(two_a)
        three_a.fold()
        do_up(1)
        three_a.halve()
        three_b = Reduce(d_pre[1], w_up, True, "three_b")
        do_mid_bwd(0, three_a)
        two_b = do_down(1)
        three_b.fold()
        do_y(0, sum_two_a)
        d_down = done(weight_grad([turn(hidden[0]), hidden[1]], [(grad_y, c) for c in chunks], 1280, 1280, "d_down"))
        three_b.halve()
        d_attn = [None] * 2
        d_attn[0] = done(mm("se,ce->sc", turn(d_resid[0]), w_proj).astype(BF))
        layer_out = done(place(turn(y_full[0]), 0, tokens, [], "y_place_0"))
        do_mid_bwd(1, three_b)
        sum_two_b = scatter(turn(two_b))
        d_up = done(weight_grad([turn(normed_two[0]), normed_two[1]], d_pre, 1280, 1280, "d_up"))
        d_attn[1] = done(mm("se,ce->sc", turn(d_resid[1]), w_proj).astype(BF))
        later = do_attn_bwd(1, [])
        four_b = Reduce(d_qkv[1], w_qkv, True, "four_b")
        do_attn_bwd(0, later)
        do_y(1, sum_two_b)
        four_b.fold()
        four_a = Reduce(d_qkv[0], w_qkv, True, "four_a")
        four_b.halve()
        d_wout = done(weight_grad([turn(attn[0]), attn[1]], d_resid, heads * dim, 1280, "d_wout"))
        do_in_bwd(1, four_b)
        four_a.fold()
        d_wqkv = done(weight_grad([turn(normed_one[0]), normed_one[1]], d_qkv, 1024, 3 * heads * dim, "d_wqkv_0", 0, 3))
        four_a.halve()
        layer_out = done(place(turn(y_full[1]), rows, tokens, [layer_out], "y_place_1"))
        do_in_bwd(0, four_a)
        dg = jnp.concatenate([dg_one[0] + dg_one[1], dg_two[0] + dg_two[1]], axis=0)
        d_wqkv = done(weight_grad([turn(normed_one[0]), normed_one[1]], d_qkv, 1024, 3 * heads * dim, "d_wqkv_1", 3, 2,
                                  [d_wqkv]))
        grad_x = done(place(turn(x_new[1]), rows, tokens, [], "x_place_1"))
        for step in (1, 2, 4):
            dg = dg + lax.ppermute(dg, "model", [(i, i ^ step) for i in range(n_dev)])
        grad_x = place(turn(x_new[0]), 0, tokens, [grad_x], "x_place_0")
        dg = dg.astype(BF)
        return layer_out, grad_x, d_wqkv, d_wout.reshape(heads, dim, width), d_up, d_down, dg[0], dg[1]

    in_specs = (P("data", None), P("data"), P(None), P(None), P(None, "model"),
                P("model", None, None), P(None, "model"), P("model", None), P("data", None))
    out_specs = (P("data", None), P("data", None), P("data", "model"), P(("data", "model"), None, None),
                 P("data", "model"), P(("data", "model"), None), P("data"), P("data"))
    return jax.shard_map(local_layer, mesh=mesh, in_specs=in_specs, out_specs=out_specs, check_vma=False)
```

```python
import functools
import jax
import jax.numpy as jnp
from jax import lax
from jax.experimental import pallas as pl
from jax.experimental.pallas import tpu as pltpu
from jax.sharding import PartitionSpec as P


LN_EPS = 1e-5
TILE = 256
BF = jnp.bfloat16
F32 = jnp.float32
gelu_tanh = functools.partial(jax.nn.gelu, approximate=True)


def mm(spec, left, right):
    return jnp.einsum(spec, left, right, preferred_element_type=F32)


def normalize(values):
    values_f32 = values.astype(F32)
    centered = values_f32 - jnp.mean(values_f32, axis=-1, keepdims=True)
    inv_std = lax.rsqrt(jnp.mean(centered * centered, axis=-1, keepdims=True) + LN_EPS)
    return centered * inv_std, inv_std


def norm_backward(grad_out, x_hat, inv_std, gain_vec):
    d_gain = jnp.sum(grad_out * x_hat, axis=0)
    d_hat = grad_out * gain_vec.astype(F32)
    d_in = inv_std * (d_hat - jnp.mean(d_hat, axis=-1, keepdims=True)
                      - x_hat * jnp.mean(d_hat * x_hat, axis=-1, keepdims=True))
    return d_in, d_gain


def dot_nt(left, right):
    return lax.dot_general(left, right, (((1,), (1,)), ((), ())), preferred_element_type=F32)


def dot_tn(left, right):
    return lax.dot_general(left, right, (((0,), (0,)), ((), ())), preferred_element_type=F32)


def dot_nn(left, right):
    return lax.dot_general(left, right, (((1,), (0,)), ((), ())), preferred_element_type=F32)


def scores_t(keys, query, segk_ref, segq, k_start, diagonal):
    block = dot_nt(keys, query) * (query.shape[-1] ** -0.5)
    seen = segk_ref[k_start:k_start + TILE, :] == segq
    if diagonal:
        seen = seen & (lax.broadcasted_iota(jnp.int32, (TILE, TILE), 0)
                       <= lax.broadcasted_iota(jnp.int32, (TILE, TILE), 1))
    return jnp.where(seen, block, -1e30)


def key_blocks(prev, cur, rows, tile, first):
    out = []
    for c, ref in enumerate(prev):
        out += [(ref, r, c * rows + r) for r in range(0, rows, TILE)]
    out += [(cur, r, first + r) for r in range(0, (tile + 1) * TILE, TILE)]
    return out


def attn_fwd_kernel(n_prev, rows, dim, *refs):
    segk_ref, segq_ref = refs[:2]
    prev, cur = refs[2:2 + n_prev], refs[2 + n_prev]
    o_ref, stat_ref, s_ref, p_ref = refs[3 + n_prev:]
    first = n_prev * rows
    for t in range(rows // TILE):
        lo = t * TILE
        query = cur[lo:lo + TILE, 0:dim]
        segq = segq_ref[:, first + lo:first + lo + TILE]
        blocks = key_blocks(prev, cur, rows, t, first)
        top = None
        for n, (ref, r, start) in enumerate(blocks):
            block = scores_t(ref[r:r + TILE, dim:2 * dim], query, segk_ref, segq, start, n == len(blocks) - 1)
            s_ref[n * TILE:(n + 1) * TILE, :] = block
            here = jnp.max(block, axis=0, keepdims=True)
            top = here if top is None else jnp.maximum(top, here)
        total = None
        for n in range(len(blocks)):
            expd = jnp.exp(s_ref[n * TILE:(n + 1) * TILE, :] - top)
            s_ref[n * TILE:(n + 1) * TILE, :] = expd
            here = jnp.sum(expd, axis=0, keepdims=True)
            total = here if total is None else total + here
        inv = 1.0 / total
        for n in range(len(blocks)):
            p_ref[n * TILE:(n + 1) * TILE, :] = (s_ref[n * TILE:(n + 1) * TILE, :] * inv).astype(BF)
        out_t = dot_tn(cur[0:lo + TILE, 2 * dim:3 * dim], p_ref[first:first + lo + TILE, :])
        for c, ref in enumerate(prev):
            out_t = out_t + dot_tn(ref[:, 2 * dim:3 * dim], p_ref[c * rows:(c + 1) * rows, :])
        o_ref[lo:lo + TILE, :] = out_t.T.astype(BF)
        stat_ref[0, 0:1, lo:lo + TILE] = top
        stat_ref[0, 1:2, lo:lo + TILE] = inv


def attn_bwd_kernel(n_prev, n_later, rows, dim, *refs):
    segk_ref, segq_ref = refs[:2]
    prev, cur = refs[2:2 + n_prev], refs[2 + n_prev]
    do_ref, stat_ref = refs[3 + n_prev:5 + n_prev]
    later = refs[5 + n_prev:5 + n_prev + n_later]
    rest = refs[5 + n_prev + n_later:]
    dqkv_ref, dkv_prev = rest[0], rest[1:1 + n_prev]
    p_ref, dp_ref, ds_ref, acc_k, acc_v = rest[1 + n_prev:]
    first = n_prev * rows
    scale = dim ** -0.5
    acc_k[...] = jnp.zeros_like(acc_k)
    acc_v[...] = jnp.zeros_like(acc_v)
    for ref in later:
        acc_k[first:first + rows, :] += ref[:, 0:dim]
        acc_v[first:first + rows, :] += ref[:, dim:2 * dim]
    for t in range(rows // TILE):
        lo = t * TILE
        query = cur[lo:lo + TILE, 0:dim]
        d_out = do_ref[lo:lo + TILE, :]
        segq = segq_ref[:, first + lo:first + lo + TILE]
        top = stat_ref[0, 0:1, lo:lo + TILE]
        inv = stat_ref[0, 1:2, lo:lo + TILE]
        blocks = key_blocks(prev, cur, rows, t, first)
        delta = jnp.zeros_like(top)
        for n, (ref, r, start) in enumerate(blocks):
            block = scores_t(ref[r:r + TILE, dim:2 * dim], query, segk_ref, segq, start, n == len(blocks) - 1)
            prob = jnp.exp(block - top) * inv
            d_prob = dot_nt(ref[r:r + TILE, 2 * dim:3 * dim], d_out).astype(BF)
            delta += jnp.sum(prob * d_prob.astype(F32), axis=0, keepdims=True)
            p_ref[n * TILE:(n + 1) * TILE, :] = prob
            dp_ref[n * TILE:(n + 1) * TILE, :] = d_prob
        for n in range(len(blocks)):
            span = slice(n * TILE, (n + 1) * TILE)
            prob = p_ref[span, :]
            d_score = (prob * (dp_ref[span, :].astype(F32) - delta) * scale).astype(BF)
            ds_ref[span, :] = d_score
            acc_v[span, :] += dot_nn(prob.astype(BF), d_out)
            acc_k[span, :] += dot_nn(d_score, query)
        dq_t = dot_tn(cur[0:lo + TILE, dim:2 * dim], ds_ref[first:first + lo + TILE, :])
        for c, ref in enumerate(prev):
            dq_t = dq_t + dot_tn(ref[:, dim:2 * dim], ds_ref[c * rows:(c + 1) * rows, :])
        dqkv_ref[lo:lo + TILE, 0:dim] = dq_t.T.astype(BF)
    dqkv_ref[:, dim:2 * dim] = acc_k[first:first + rows, :].astype(BF)
    dqkv_ref[:, 2 * dim:3 * dim] = acc_v[first:first + rows, :].astype(BF)
    for c, ref in enumerate(dkv_prev):
        ref[:, 0:dim] = acc_k[c * rows:(c + 1) * rows, :]
        ref[:, dim:2 * dim] = acc_v[c * rows:(c + 1) * rows, :]


def whole(shape):
    return pl.BlockSpec(shape, lambda h: (0,) * len(shape))


def by_head(rows, cols):
    return pl.BlockSpec((rows, cols), lambda h: (0, h))


def attention_fwd(segk, segq, qkv_prev, qkv_cur, heads, dim):
    rows, n_prev = qkv_cur.shape[0], len(qkv_prev)
    keys = (n_prev + 1) * rows
    return pl.pallas_call(
        functools.partial(attn_fwd_kernel, n_prev, rows, dim),
        grid=(heads,),
        in_specs=[whole(segk.shape), whole(segq.shape)] + [by_head(rows, 3 * dim)] * (n_prev + 1),
        out_specs=[by_head(rows, dim), pl.BlockSpec((1, 2, rows), lambda h: (h, 0, 0))],
        out_shape=[jax.ShapeDtypeStruct((rows, heads * dim), BF), jax.ShapeDtypeStruct((heads, 2, rows), F32)],
        scratch_shapes=[pltpu.VMEM((keys, TILE), F32), pltpu.VMEM((keys, TILE), BF)],
    )(segk, segq, *qkv_prev, qkv_cur)


def attention_bwd(segk, segq, qkv_prev, qkv_cur, d_out, stats, later, heads, dim):
    rows, n_prev = qkv_cur.shape[0], len(qkv_prev)
    keys = (n_prev + 1) * rows
    return pl.pallas_call(
        functools.partial(attn_bwd_kernel, n_prev, len(later), rows, dim),
        grid=(heads,),
        in_specs=[whole(segk.shape), whole(segq.shape)] + [by_head(rows, 3 * dim)] * (n_prev + 1)
        + [by_head(rows, dim), pl.BlockSpec((1, 2, rows), lambda h: (h, 0, 0))] + [by_head(rows, 2 * dim)] * len(later),
        out_specs=[by_head(rows, 3 * dim)] + [by_head(rows, 2 * dim)] * n_prev,
        out_shape=[jax.ShapeDtypeStruct((rows, 3 * heads * dim), BF)]
        + [jax.ShapeDtypeStruct((rows, 2 * heads * dim), F32)] * n_prev,
        scratch_shapes=[pltpu.VMEM((keys, TILE), F32), pltpu.VMEM((keys, TILE), BF), pltpu.VMEM((keys, TILE), BF),
                        pltpu.VMEM((keys, dim), F32), pltpu.VMEM((keys, dim), F32)],
    )(segk, segq, *qkv_prev, qkv_cur, d_out, stats, *later)


def wgrad_kernel(n, *refs):
    out = dot_tn(refs[0][...], refs[n][...])
    for c in range(1, n):
        out += dot_tn(refs[c][...], refs[n + c][...])
    refs[-1][...] = out.astype(BF)


def weight_grad(lefts, rights, tile_m, tile_n, first=0, count=None, into=()):
    n, rows = len(lefts), lefts[0].shape[0]
    rights = [r if isinstance(r, tuple) else (r, 0) for r in rights]
    m_dim, n_dim = lefts[0].shape[1], rights[0][0].shape[1]
    count = count or m_dim // tile_m - first
    in_specs = [pl.BlockSpec((rows, tile_m), lambda i, j: (0, i + first)) for _ in lefts]
    in_specs += [pl.BlockSpec((rows, tile_n), functools.partial(lambda b, i, j: (b, j), b)) for _, b in rights]
    return pl.pallas_call(
        functools.partial(wgrad_kernel, n),
        grid=(count, n_dim // tile_n),
        in_specs=in_specs + [pl.BlockSpec(memory_space=pl.ANY)] * len(into),
        out_specs=pl.BlockSpec((tile_m, tile_n), lambda i, j: (i + first, j)),
        out_shape=jax.ShapeDtypeStruct((m_dim, n_dim), BF),
        input_output_aliases={2 * n: 0} if into else {},
        compiler_params=pltpu.CompilerParams(vmem_limit_bytes=56 * 1024 * 1024),
    )(*lefts, *[r for r, _ in rights], *into)


GROUP = 16


def groups(ref):
    return [slice(r, r + GROUP) for r in range(0, ref.shape[0], GROUP)]


def total_of(refs, span):
    return sum([ref[span, :].astype(F32) for ref in refs[1:]], refs[0][span, :].astype(F32))


def ln_fwd_kernel(x_ref, gain_ref, o_ref):
    for span in groups(x_ref):
        hat, _ = normalize(x_ref[span, :])
        o_ref[span, :] = (hat * gain_ref[...].astype(F32)).astype(BF)


def ln_mid_kernel(_, x_ref, *refs):
    parts, (gain_ref, x1_ref, o_ref) = refs[:-3], refs[-3:]
    for span in groups(x_ref):
        resid = (x_ref[span, :].astype(F32) + total_of(parts, span)).astype(BF)
        x1_ref[span, :] = resid
        hat, _ = normalize(resid)
        o_ref[span, :] = (hat * gain_ref[...].astype(F32)).astype(BF)


def ln_bwd_kernel(_, x_ref, *refs):
    parts, (gain_ref, resid_ref, o_ref, dg_ref) = refs[:-4], refs[-4:]

    @pl.when(pl.program_id(0) == 0)
    def _():
        dg_ref[...] = jnp.zeros_like(dg_ref)

    for span in groups(x_ref):
        hat, inv_std = normalize(x_ref[span, :])
        d_normed = total_of(parts, span).astype(BF).astype(F32)
        d_in, d_gain = norm_backward(d_normed, hat, inv_std, gain_ref[...])
        o_ref[span, :] = (resid_ref[span, :].astype(F32) + d_in).astype(BF)
        dg_ref[...] += d_gain[None, :]


def add_kernel(_, x_ref, sum_ref, o_ref):
    o_ref[...] = (x_ref[...].astype(F32) + sum_ref[...].astype(F32)).astype(BF)


def part_kernel(own, transposed, order_ref, act_ref, w_ref, far_ref, near_ref, rows_ref):
    n = act_ref.shape[0] // own

    @pl.when(pl.program_id(0) == 0)
    def _():
        for p in range(n):
            rows_ref[p * own:(p + 1) * own, :] = act_ref[pl.ds(pl.multiple_of(order_ref[p] * own, 16), own), :]

    total = (dot_nt if transposed else dot_nn)(rows_ref[...], w_ref[...]).astype(BF)
    far_ref[...] = total[:n // 2 * own]
    near_ref[...] = total[n // 2 * own:]


def part_call(order, act, weight, own, transposed, tile=512):
    rows, depth = act.shape
    width = weight.shape[0 if transposed else 1]
    w_spec = (pl.BlockSpec((tile, depth), lambda i: (i, 0)) if transposed
              else pl.BlockSpec((depth, tile), lambda i: (0, i)))
    half = pl.BlockSpec((rows // 2, tile), lambda i: (0, i))
    return pl.pallas_call(
        functools.partial(part_kernel, own, transposed),
        grid=(width // tile,),
        in_specs=[pl.BlockSpec(memory_space=pltpu.SMEM), pl.BlockSpec((rows, depth), lambda i: (0, 0)), w_spec],
        out_specs=[half, half],
        out_shape=[jax.ShapeDtypeStruct((rows // 2, width), BF)] * 2,
        scratch_shapes=[pltpu.VMEM((rows, depth), BF)],
    )(order, act, weight)


def fold_kernel(own, part_ref, got_ref, *out_refs):
    for p, out_ref in enumerate(out_refs):
        span = slice(p * own, (p + 1) * own)
        out_ref[...] = (part_ref[span, :].astype(F32) + got_ref[span, :].astype(F32)).astype(BF)


def place_kernel(x_ref, *refs):
    refs[-1][...] = x_ref[...]


def col_call(kernel, head, arrays, out_rows, tile=1280):
    width = arrays[0].shape[1]
    spec = lambda r: pl.BlockSpec((r, tile), lambda i: (0, i))
    return pl.pallas_call(
        kernel,
        grid=(width // tile,),
        in_specs=[pl.BlockSpec(memory_space=pltpu.SMEM)] * len(head) + [spec(a.shape[0]) for a in arrays],
        out_specs=[spec(r) for r in out_rows],
        out_shape=[jax.ShapeDtypeStruct((r, width), BF) for r in out_rows],
    )(*head, *arrays)


def place(block, start, total, into, tile=256):
    rows, width = block.shape
    first = start // tile
    return pl.pallas_call(
        place_kernel,
        grid=(rows // tile,),
        in_specs=[pl.BlockSpec((tile, width), lambda i: (i, 0))] + [pl.BlockSpec(memory_space=pl.ANY)] * len(into),
        out_specs=pl.BlockSpec((tile, width), lambda i: (i + first, 0)),
        out_shape=jax.ShapeDtypeStruct((total, width), BF),
        input_output_aliases={1: 0} if into else {},
    )(block, *into)


def ln_call(array, gain, rows, start, tile=64):
    width, first = array.shape[1], start // tile
    return pl.pallas_call(
        ln_fwd_kernel,
        grid=(rows // tile,),
        in_specs=[pl.BlockSpec((tile, width), lambda i: (i + first, 0)), pl.BlockSpec((1, width), lambda i: (0, 0))],
        out_specs=pl.BlockSpec((tile, width), lambda i: (i, 0)),
        out_shape=jax.ShapeDtypeStruct((rows, width), BF),
    )(array, gain)


def row_call(kernel, place_of, arrays, outs, own, tile=32):
    width, steps = arrays[0].shape[1], own // tile

    def spec(rows):
        if rows == 1:
            return pl.BlockSpec((1, width), lambda i, at: (0, 0))
        if rows == own:
            return pl.BlockSpec((tile, width), lambda i, at: (i, 0))
        return pl.BlockSpec((tile, width), lambda i, at: (at[0] * steps + i, 0))

    return pl.pallas_call(
        kernel,
        grid_spec=pltpu.PrefetchScalarGridSpec(
            num_scalar_prefetch=1, grid=(steps,),
            in_specs=[spec(a.shape[0]) for a in arrays], out_specs=[spec(r) for r, _ in outs]),
        out_shape=[jax.ShapeDtypeStruct((r, width), d) for r, d in outs],
    )(place_of, *arrays)


def after(value, *deps):
    return lax.optimization_barrier((value, *deps))[0]


N_CHUNKS = 2


def solution(mesh):
    n_dev = mesh.shape["model"]

    def layer(act_x, seg_ids, gain_one, gain_two, w_qkv, w_out, w_up, w_down, grad_y):
        tokens, width = act_x.shape
        heads, dim = w_out.shape[0], w_out.shape[1]
        w_proj = w_out.reshape(heads * dim, width)
        rows = tokens // N_CHUNKS
        own = rows // n_dev
        me = lax.axis_index("model")
        chunks = range(N_CHUNKS)

        def chunk_of(array, c):
            return array[c * rows:(c + 1) * rows]

        def gather_rows(block):
            return lax.all_gather(block, "model", axis=0, tiled=True)

        core, x_bit, y_bit = me % 2, (me // 2) % 2, me // 4
        swap_core = [(i, i ^ 1) for i in range(n_dev)]
        here = y_bit * 2 + x_bit
        order = jnp.stack([(here ^ k) * 2 + which for which in (1 - core, core) for k in (3, 1, 2, 0)]).astype(jnp.int32)
        own_at = [(me + c * n_dev).reshape(1).astype(jnp.int32) for c in chunks]

        segk = jnp.broadcast_to(seg_ids[:, None], (tokens, TILE))
        segq = seg_ids[None, :]
        gain_one, gain_two = gain_one[None, :], gain_two[None, :]
        last = [seg_ids]

        def turn(value, *deps):
            return after(value, last[0], *deps)

        def done(value):
            last[0] = value
            return value

        class Reduce:
            def __init__(self, act, weight, transposed):
                part, self.part = part_call(order, turn(act), weight, own, transposed)
                done(part)
                self.got = lax.ppermute(part, "model", swap_core)

            def arrive(self):
                self.got = done(turn(self.got))

            def fold(self):
                *sends, keep = col_call(functools.partial(fold_kernel, own), [], [turn(self.part), self.got], [own] * 4)
                done(keep)
                self.parts = [keep]
                for send, step in zip(sends, (6, 2, 4)):
                    self.parts.append(lax.ppermute(send, "model", [(i, i ^ step) for i in range(n_dev)]))

        normed_one, qkv, attn, stats = [None] * 2, [None] * 2, [None] * 2, [None] * 2
        x1_own, normed_two, d_hidden, hidden, d_pre = [None] * 2, [None] * 2, [None] * 2, [None] * 2, [None] * 2
        d_resid_own, d_resid, d_attn, d_qkv = [None] * 2, [None] * 2, [None] * 2, [None] * 2
        dg_two, dg_one, y_full, x_new = [None] * 2, [None] * 2, [None] * 2, [None] * 2

        def do_norm(c):
            normed_one[c] = done(ln_call(turn(act_x), gain_one, rows, c * rows))

        def do_qkv(c):
            qkv[c] = done(mm("sh,hc->sc", turn(normed_one[c]), w_qkv).astype(BF))

        def do_attn(c):
            out, stats[c] = attention_fwd(segk, turn(segq), qkv[:c], qkv[c], heads, dim)
            attn[c] = done(out)

        def do_d_hidden(c):
            d_hidden[c] = done(after(mm("se,fe->sf", chunk_of(turn(grad_y), c), w_down).astype(BF)))

        def do_mid(c, red):
            x1_own[c], block = row_call(
                ln_mid_kernel, own_at[c], [turn(act_x), *red.parts, gain_two], [(own, BF)] * 2, own)
            normed_two[c] = gather_rows(done(block))

        def do_up(c):
            pre_act = mm("sh,hf->sf", turn(normed_two[c]), w_up)
            act_vals, gelu_pull = jax.vjp(gelu_tanh, pre_act)
            hidden[c] = act_vals.astype(BF)
            d_pre[c] = done(gelu_pull(d_hidden[c].astype(F32))[0].astype(BF))

        def do_mid_bwd(c, red):
            d_resid_own[c], dg_two[c] = row_call(
                ln_bwd_kernel, own_at[c], [turn(x1_own[c]), *red.parts, gain_two, grad_y], [(own, BF), (1, F32)], own)
            d_resid[c] = gather_rows(done(d_resid_own[c]))

        def do_attn_bwd(c, later):
            outs = attention_bwd(segk, turn(segq), qkv[:c], qkv[c], d_attn[c], stats[c], later, heads, dim)
            d_qkv[c] = done(outs[0])
            return outs[1:]

        def do_y(c, red):
            y_own = done(row_call(add_kernel, own_at[c], [turn(x1_own[c]), red], [(own, BF)], own)[0])
            y_full[c] = gather_rows(y_own)

        def do_in_bwd(c, red):
            block, dg_one[c] = row_call(
                ln_bwd_kernel, own_at[c], [turn(act_x), *red.parts, gain_one, d_resid_own[c]], [(own, BF), (1, F32)], own)
            x_new[c] = gather_rows(done(block))

        def do_down(c):
            return done(mm("sf,fe->se", turn(hidden[c]), w_down).astype(BF))

        def scatter(part):
            return lax.psum_scatter(part, "model", scatter_dimension=0, tiled=True)

        do_norm(0)
        do_qkv(0)
        do_attn(0)
        one_a = Reduce(attn[0], w_proj, False)
        do_norm(1)
        one_a.fold()
        do_qkv(1)
        do_attn(1)
        one_b = Reduce(attn[1], w_proj, False)
        do_mid(0, one_a)
        do_d_hidden(0)
        one_b.fold()
        do_d_hidden(1)
        do_up(0)
        do_mid(1, one_b)
        three_a = Reduce(d_pre[0], w_up, True)
        two_a = do_down(0)
        three_a.fold()
        sum_two_a = scatter(after(two_a, last[0]))
        do_up(1)
        three_b = Reduce(d_pre[1], w_up, True)
        do_mid_bwd(0, three_a)
        do_y(0, sum_two_a)
        two_b = do_down(1)
        three_b.fold()
        d_down = done(weight_grad([turn(hidden[0]), hidden[1]], [(grad_y, c) for c in chunks], 1280, 1280))
        d_attn = [None] * 2
        d_attn[0] = done(mm("se,ce->sc", turn(d_resid[0]), w_proj).astype(BF))
        layer_out = done(place(turn(y_full[0]), 0, tokens, []))
        do_mid_bwd(1, three_b)
        sum_two_b = scatter(turn(two_b))
        d_up = done(weight_grad([turn(normed_two[0]), normed_two[1]], d_pre, 1280, 1280))
        d_attn[1] = done(mm("se,ce->sc", turn(d_resid[1]), w_proj).astype(BF))
        later = do_attn_bwd(1, [])
        four_b = Reduce(d_qkv[1], w_qkv, True)
        do_attn_bwd(0, later)
        four_b.fold()
        do_y(1, sum_two_b)
        four_a = Reduce(d_qkv[0], w_qkv, True)
        d_wqkv = done(weight_grad([turn(normed_one[0]), normed_one[1]], d_qkv, 1024, 3 * heads * dim, 0, 3))
        four_a.arrive()
        do_in_bwd(1, four_b)
        four_a.fold()
        d_wqkv = done(weight_grad([turn(normed_one[0]), normed_one[1]], d_qkv, 1024, 3 * heads * dim, 3, 2,
                                  [d_wqkv]))
        d_wout = done(weight_grad([turn(attn[0]), attn[1]], d_resid, heads * dim, 1280))
        layer_out = done(place(turn(y_full[1]), rows, tokens, [layer_out]))
        do_in_bwd(0, four_a)
        dg = jnp.concatenate([dg_one[0] + dg_one[1], dg_two[0] + dg_two[1]], axis=0)
        grad_x = done(place(turn(x_new[1]), rows, tokens, []))
        for step in (1, 2, 4):
            dg = dg + lax.ppermute(dg, "model", [(i, i ^ step) for i in range(n_dev)])
        grad_x = place(turn(x_new[0]), 0, tokens, [grad_x])
        dg = dg.astype(BF)
        return layer_out, grad_x, d_wqkv, d_wout.reshape(heads, dim, width), d_up, d_down, dg[0], dg[1]

    in_specs = (P("data", None), P("data"), P(None), P(None), P(None, "model"),
                P("model", None, None), P(None, "model"), P("model", None), P("data", None))
    out_specs = (P("data", None), P("data", None), P("data", "model"), P(("data", "model"), None, None),
                 P("data", "model"), P(("data", "model"), None), P("data"), P("data"))
    return jax.shard_map(layer, mesh=mesh, in_specs=in_specs, out_specs=out_specs, check_vma=False)
```
